16 devices in a mesh: dp: 2 (over y, z), tp: 8 (over x, core).
Axes of the slice: x: 4, y: 2, z: 1, core: 2. Of those that a mesh axis runs over, the one named last changes fastest.
The devices are a block of a 4x4x8 slice.
Arguments:
- hidden: bfloat16 [64, 1536], P('dp'), parts along dimension 0
- lengths: int32 [64], P('dp'), parts along dimension 0
- choice: int32 [2, 64, 8], P(None, 'dp'), parts along dimension 1
- keys_one: bfloat16 [64, 128, 8, 64], P('dp', 'tp'), parts along dimension 0
- vals_one: bfloat16 [64, 128, 8, 64], P('dp', 'tp'), parts along dimension 0
- keys_two: bfloat16 [64, 128, 8, 64], P('dp', 'tp'), parts along dimension 0
- vals_two: bfloat16 [64, 128, 8, 64], P('dp', 'tp'), parts along dimension 0
- g_attn: bfloat16 [2, 1536], replicated
- w_q: bfloat16 [2, 1536, 1536], P(None, None, 'tp')
- w_k: bfloat16 [2, 1536, 512], P(None, None, 'tp')
- w_v: bfloat16 [2, 1536, 512], P(None, None, 'tp')
- w_o: bfloat16 [2, 1536, 1536], P(None, 'tp')
- g_mlp: bfloat16 [2, 1536], replicated
- w_router: bfloat16 [2, 1536, 40], replicated
- w_gate: bfloat16 [2, 40, 1536, 512], P(None, None, None, 'tp')
- w_up: bfloat16 [2, 40, 1536, 512], P(None, None, None, 'tp')
- w_down: bfloat16 [2, 40, 512, 1536], P(None, None, 'tp')
Outputs:
- output 1: bfloat16 [64, 1536], P('dp'), parts along dimension 0
- output 2: bfloat16 [64, 128, 8, 64], P('dp', None, 'tp'), parts along dimension 0
- output 3: bfloat16 [64, 128, 8, 64], P('dp', None, 'tp'), parts along dimension 0
- output 4: bfloat16 [64, 128, 8, 64], P('dp', None, 'tp'), parts along dimension 0
- output 5: bfloat16 [64, 128, 8, 64], P('dp', None, 'tp'), parts along dimension 0
There are 2 independent parts. The reference program is written for one: setup_inputs(seed, part) draws one part's arguments, and reference() takes and returns one part's arrays. A program takes and returns all parts, laid end to end along the dimension named above; an argument that names none is the same for every part.
All inputs are finite; a program needn't handle non-finite values.
Results may differ from the reference program's by a relative error of at most 0.02.
Values are sent between devices in bfloat16 or wider.
A program may use at most 768 MiB of HBM per device.

```python
import jax
import jax.numpy as jnp
from jax import lax

BATCH = 32
SEQ = 128
D = 1536
HEADS = 24
KV_HEADS = 8
HEAD = 64
FF = 512
EXPERTS = 40
TOP = 8
LAYERS = 2
EPS = 1e-5
THETA = 1000000.0


def weight_draw(key, shape, fan_in, gain_mult):
    return (jax.random.normal(key, shape, jnp.float32) * (gain_mult * fan_in ** -0.5)).astype(jnp.bfloat16)


def value_walk(key, cache_shape):
    step_key, noise_key = jax.random.split(key)
    walk_steps = jax.random.normal(step_key, cache_shape, jnp.float32) * SEQ ** -0.5
    noise_part = 0.5 * jax.random.normal(noise_key, cache_shape, jnp.float32)
    return (jnp.cumsum(walk_steps, axis=1) + noise_part).astype(jnp.bfloat16)


def setup_inputs(seed: int = 0, part: int = 0) -> dict:
    base_key = jax.random.key(seed)
    shared = jax.random.split(base_key, 11)
    local_keys = jax.random.split(jax.random.fold_in(base_key, part), 9)
    cache_shape = (BATCH, SEQ, KV_HEADS, HEAD)
    hidden = jax.random.normal(local_keys[0], (BATCH, D), jnp.float32).astype(jnp.bfloat16)
    drawn_lens = jax.random.randint(local_keys[1], (BATCH,), 0, SEQ)
    full_row = jax.random.randint(local_keys[2], (), 0, BATCH)
    lengths = jnp.where(jnp.arange(BATCH) == full_row, SEQ - 1, drawn_lens).astype(jnp.int32)
    rank_score = jax.random.randint(local_keys[3], (LAYERS, BATCH, EXPERTS), 0, 2 ** 20) * EXPERTS + jnp.arange(EXPERTS)
    choice = lax.top_k(rank_score, TOP)[1].astype(jnp.int32)
    return {
        'hidden': hidden,
        'lengths': lengths,
        'choice': choice,
        'keys_one': jax.random.normal(local_keys[4], cache_shape, jnp.float32).astype(jnp.bfloat16),
        'vals_one': value_walk(local_keys[5], cache_shape),
        'keys_two': jax.random.normal(local_keys[6], cache_shape, jnp.float32).astype(jnp.bfloat16),
        'vals_two': value_walk(local_keys[7], cache_shape),
        'g_attn': (1.0 + 0.3 * jax.random.normal(shared[0], (LAYERS, D), jnp.float32)).astype(jnp.bfloat16),
        'w_q': weight_draw(shared[1], (LAYERS, D, HEADS * HEAD), D, 1.0),
        'w_k': weight_draw(shared[2], (LAYERS, D, KV_HEADS * HEAD), D, 1.0),
        'w_v': weight_draw(shared[3], (LAYERS, D, KV_HEADS * HEAD), D, 1.0),
        'w_o': weight_draw(shared[4], (LAYERS, HEADS * HEAD, D), HEADS * HEAD, 1.0),
        'g_mlp': (1.0 + 0.3 * jax.random.normal(shared[5], (LAYERS, D), jnp.float32)).astype(jnp.bfloat16),
        'w_router': weight_draw(shared[6], (LAYERS, D, EXPERTS), D, 2.0),
        'w_gate': weight_draw(shared[7], (LAYERS, EXPERTS, D, FF), D, 1.0),
        'w_up': weight_draw(shared[8], (LAYERS, EXPERTS, D, FF), D, 1.0),
        'w_down': weight_draw(shared[9], (LAYERS, EXPERTS, FF, D), FF, 2.0),
    }


def rms_norm(tensor, gain_vec):
    tensor_f = tensor.astype(jnp.float32)
    scale = lax.rsqrt(jnp.mean(tensor_f * tensor_f, axis=-1, keepdims=True) + EPS)
    return (tensor_f * scale * gain_vec.astype(jnp.float32)).astype(jnp.bfloat16)


def apply_rope(tensor, lengths):
    head_dim = tensor.shape[-1]
    half_dim = head_dim // 2
    inv_freq = THETA ** (-2.0 * jnp.arange(half_dim, dtype=jnp.float32) / head_dim)
    angle = lengths.astype(jnp.float32)[:, None] * inv_freq[None, :]
    cos_part = jnp.cos(angle)[:, None, :]
    sin_part = jnp.sin(angle)[:, None, :]
    lower_half = tensor[..., :half_dim]
    upper_half = tensor[..., half_dim:]
    return jnp.concatenate([lower_half * cos_part - upper_half * sin_part, upper_half * cos_part + lower_half * sin_part], axis=-1)


def decode_layer(hidden, lengths, choice, key_cache, val_cache, g_attn, w_q, w_k, w_v, w_o, g_mlp, w_router, w_gate, w_up, w_down):
    batch_rows = hidden.shape[0]
    seq_len = key_cache.shape[1]
    normed = rms_norm(hidden, g_attn)
    query_rot = apply_rope(jnp.dot(normed, w_q, preferred_element_type=jnp.float32).reshape(batch_rows, HEADS, HEAD), lengths).astype(jnp.bfloat16)
    key_new = apply_rope(jnp.dot(normed, w_k, preferred_element_type=jnp.float32).reshape(batch_rows, KV_HEADS, HEAD), lengths).astype(jnp.bfloat16)
    val_new = jnp.dot(normed, w_v, preferred_element_type=jnp.float32).astype(jnp.bfloat16).reshape(batch_rows, KV_HEADS, HEAD)
    positions = jnp.arange(seq_len)
    is_new = (positions[None, :] == lengths[:, None])[:, :, None, None]
    key_cache = jnp.where(is_new, key_new[:, None], key_cache)
    val_cache = jnp.where(is_new, val_new[:, None], val_cache)
    query_grp = query_rot.reshape(batch_rows, KV_HEADS, HEADS // KV_HEADS, HEAD)
    scores = jnp.einsum('bgrd,bsgd->bgrs', query_grp.astype(jnp.float32), key_cache.astype(jnp.float32)) * HEAD ** -0.5
    is_valid = (positions[None, :] <= lengths[:, None])[:, None, None, :]
    attn_prob = jax.nn.softmax(jnp.where(is_valid, scores, -1e30), axis=-1).astype(jnp.bfloat16)
    attn_vec = jnp.einsum('bgrs,bsgd->bgrd', attn_prob.astype(jnp.float32), val_cache.astype(jnp.float32)).astype(jnp.bfloat16).reshape(batch_rows, HEADS * HEAD)
    x_mid = (hidden.astype(jnp.float32) + jnp.dot(attn_vec, w_o, preferred_element_type=jnp.float32)).astype(jnp.bfloat16)
    normed_mid = rms_norm(x_mid, g_mlp)
    logits = jnp.dot(normed_mid, w_router, preferred_element_type=jnp.float32)
    onehot = (choice[:, :, None] == jnp.arange(EXPERTS)[None, None, :]).astype(jnp.float32)
    gate_prob = jax.nn.softmax(jnp.sum(onehot * logits[:, None, :], axis=-1), axis=-1)
    gate_mat = jnp.sum(gate_prob[:, :, None] * onehot, axis=1)
    gate_act = jnp.einsum('bd,edf->bef', normed_mid.astype(jnp.float32), w_gate.astype(jnp.float32))
    up_act = jnp.einsum('bd,edf->bef', normed_mid.astype(jnp.float32), w_up.astype(jnp.float32))
    expert_in = (jax.nn.silu(gate_act) * up_act * gate_mat[:, :, None]).astype(jnp.bfloat16)
    moe_out = jnp.einsum('bef,efd->bd', expert_in.astype(jnp.float32), w_down.astype(jnp.float32))
    return (x_mid.astype(jnp.float32) + moe_out).astype(jnp.bfloat16), key_cache, val_cache


def reference(hidden, lengths, choice, keys_one, vals_one, keys_two, vals_two, g_attn, w_q, w_k, w_v, w_o, g_mlp, w_router, w_gate, w_up, w_down):
    caches = [(keys_one, vals_one), (keys_two, vals_two)]
    results = []
    for layer_idx in range(LAYERS):
        hidden, key_cache, val_cache = decode_layer(hidden, lengths, choice[layer_idx], caches[layer_idx][0], caches[layer_idx][1], g_attn[layer_idx], w_q[layer_idx], w_k[layer_idx], w_v[layer_idx], w_o[layer_idx], g_mlp[layer_idx], w_router[layer_idx], w_gate[layer_idx], w_up[layer_idx], w_down[layer_idx])
        results.append(key_cache)
        results.append(val_cache)
    return (hidden, results[0], results[1], results[2], results[3])
```

```python
import functools

import jax
import jax.numpy as jnp
from jax import lax
from jax.experimental import pallas as pl
from jax.experimental.pallas import tpu as pltpu
from jax.sharding import PartitionSpec as P

EPS = 1e-5
THETA = 1000000.0
MESH = pl.DeviceIdType.MESH
F32 = jnp.float32
BF16 = jnp.bfloat16
CHIPS = 4
OFFSETS = ((2, 0), (2, 1), (1, 0), (3, 0), (1, 1), (3, 1), (0, 1))
CHUNKS = 10


def nt(lhs, rhs):
    return lax.dot_general(lhs, rhs, (((1,), (1,)), ((), ())), preferred_element_type=F32)


def nn(lhs, rhs):
    return jnp.dot(lhs, rhs, preferred_element_type=F32)


def iota(shape, dim):
    return lax.broadcasted_iota(jnp.int32, shape, dim)


def kernel(len_s, hid_h, choice_h, k1_h, v1_h, k2_h, v2_h, ga_h, wq_h, wk_h, wv_h, wo_h, gm_h, wr_h, wg_h, wu_h, wd_h,
           out_hid, ok1, ov1, ok2, ov2,
           hid, choice, ga, gm, xst, sendb, recvb, outst, wqkv, wo, wr, wg, wu, wd,
           qall, kdup, vdup, sc, ov, gexp, ubuf, part, d1, shot, fin,
           sem_small, sem_x, sem_w, sem_wqkv, sem_out, ss_a, rs_a, ss_r, rs_r):
    rows, dim = hid.shape
    half = dim // 2
    seq = recvb.shape[1]
    pos = seq // (2 * CHIPS)
    lanes = recvb.shape[2]
    groups = lanes // 256
    head = 64
    experts = wr.shape[1]
    step = wg.shape[1] // CHUNKS

    me = lax.axis_index("tp")
    chip, core = me // 2, lax.rem(me, 2)
    partner = chip * 2 + 1 - core

    def device(dx, flip):
        return lax.rem(chip + dx, CHIPS) * 2 + (1 - core if flip else core)

    def rcopy(src, dst, ssem, rsem, peer):
        return pltpu.make_async_remote_copy(src, dst, ssem, rsem, device_id={"tp": peer}, device_id_type=MESH)

    barrier = pltpu.get_barrier_semaphore()
    for dx, flip in OFFSETS:
        pl.semaphore_signal(barrier, inc=1, device_id={"tp": device(dx, flip)}, device_id_type=MESH)

    loads = [pltpu.make_async_copy(src, xst.at[c % 3], sem_x.at[c]) for c, src in enumerate((k1_h, v1_h, k2_h, v2_h))]
    small = [pltpu.make_async_copy(src, dst, sem_small.at[n]) for n, (src, dst) in enumerate(
        ((hid_h, hid), (choice_h, choice), (ga_h, ga), (gm_h, gm), (wr_h, wr), (wo_h, wo)))]

    def qkv_loads(layer):
        nq, nk = wq_h.shape[1], wk_h.shape[1]
        return [pltpu.make_async_copy(src.at[layer], wqkv.at[layer, pl.ds(at, size)], sem_wqkv.at[layer, n])
                for n, (src, at, size) in enumerate(((wq_h, 0, nq), (wk_h, nq, nk), (wv_h, nq + nk, nk), (wv_h, nq + 2 * nk, nk)))]

    loads[0].start()
    for copy in small[:4]:
        copy.start()
    for copy in qkv_loads(0):
        copy.start()
    loads[1].start()
    loads[2].start()
    for copy in small[4:]:
        copy.start()
    for copy in qkv_loads(1):
        copy.start()

    def w_copy(layer, which, c):
        src, dst = ((wg_h, wg), (wu_h, wu), (wd_h, wd))[which]
        at = pl.ds(pl.multiple_of(c * step, step), step)
        return pltpu.make_async_copy(src.at[layer, at], dst.at[layer, at], sem_w.at[layer, which, c])

    for layer in range(2):
        def start_weights(c, _, layer=layer):
            w_copy(layer, 0, c).start()
            w_copy(layer, 1, c).start()
            w_copy(layer, 2, c).start()
            return 0
        lax.fori_loop(0, CHUNKS, start_weights, 0)

    def permute(c):
        i, j = iota((128, 128), 0), iota((128, 128), 1)
        perm = (j == lax.rem(i, 16) * 8 + i // 16).astype(BF16)

        def body(t, _):
            tiles = [xst[c % 3, pl.ds(pl.multiple_of(t * 512 + n * 128, 128), 128), :] for n in range(4)]
            moved = nn(perm, jnp.concatenate(tiles, axis=1)).astype(BF16)
            sendb[c, :, :, pl.ds(pl.multiple_of(t * 256, 256), 256)] = moved.reshape(8, pos, 256)
            return 0
        lax.fori_loop(0, groups, body, 0)

    def a2a_copy(c, n):
        peer = device(*OFFSETS[n])
        return rcopy(sendb.at[c, peer], recvb.at[c, pl.ds(pl.multiple_of(me * pos, pos), pos)], ss_a.at[c, n], rs_a.at[c, n], peer)

    def a2a_wait(c):
        for n, (dx, flip) in reversed(list(enumerate(OFFSETS))):
            origin = device(CHIPS - dx, flip)
            rcopy(sendb.at[c, origin], recvb.at[c, pl.ds(pl.multiple_of(origin * pos, pos), pos)], ss_a.at[c, n], rs_a.at[c, n], origin).wait_recv()

    def keep_own(c):
        recvb[c, pl.ds(pl.multiple_of(me * pos, pos), pos), :] = sendb[c, me]

    loads[0].wait()
    permute(0)
    loads[3].start()
    pl.semaphore_wait(barrier, len(OFFSETS))
    for n in range(7):
        a2a_copy(0, n).start()
    loads[1].wait()
    permute(1)
    for n in range(7):
        a2a_copy(1, n).start()
    keep_own(0)
    keep_own(1)

    lane = iota((rows, 128), 1)
    row = iota((rows, 128), 0)
    len_f = jnp.zeros((rows, 128), F32)
    for b in range(rows):
        len_f = jnp.where(row == b, len_s[b].astype(F32), len_f)
    freq = jnp.exp(lax.rem(lane, 32).astype(F32) * (-2.0 / head * 13.815510557964274))
    angle = len_f * freq
    cos_t, sin_t = jnp.cos(angle), jnp.sin(angle)
    low = lax.rem(lane, head) < head // 2
    left = lane < head

    def rope(x):
        turned = jnp.where(low, -pltpu.roll(x, 96, 1), pltpu.roll(x, 32, 1))
        return (x * cos_t + turned * sin_t).astype(BF16).astype(F32)

    def norm(x, gain):
        scale = lax.rsqrt(jnp.mean(x * x, axis=-1, keepdims=True) + EPS)
        return (x * scale * gain.astype(F32)).astype(BF16)

    def project(layer, x):
        for copy in qkv_loads(layer):
            copy.wait()
        qkv = nt(norm(x, ga[layer:layer + 1, :]), wqkv[layer])
        t0, t1 = rope(qkv[:, :128]), rope(qkv[:, 128:256])
        s0, s1 = pltpu.roll(t0, 64, 1), pltpu.roll(t1, 64, 1)
        q3 = jnp.concatenate([jnp.where(left, t0, s0), jnp.where(left, s0, t0), jnp.where(left, t1, s1)], axis=0).astype(BF16)
        kdup[layer] = jnp.where(left, s1, t1)
        vdup[layer] = qkv[:, 256:384].astype(BF16).astype(F32)
        i, j = iota((128, 96), 0), iota((128, 96), 1)
        slot = lax.rem(i, 16)
        pick = (slot < 12) & (j == lax.rem(slot, 3) * rows + i // 16 * 4 + slot // 3)
        dup = nn(pick.astype(BF16), q3)
        slot2, lane2 = lax.rem(iota((128, 256), 0), 16), iota((128, 256), 1)
        both = jnp.concatenate([dup, dup], axis=1)
        qall[layer] = jnp.where(slot2 // 3 == lane2 // 64, both, 0.0).astype(BF16)

    def place_new(c, t, fresh, layer):
        at = pl.ds(pl.multiple_of(t * 256, 256), 256)
        pos_i, lane_i = iota((seq, 128), 0), iota((seq, 128), 1)
        pieces = []
        for n in range(2):
            first = t * 4 + 2 * n
            where_new = jnp.where(lane_i < head, len_s[first], len_s[first + 1])
            line = jnp.where(lane_i[:1] < head, fresh[layer, pl.ds(first, 1), :], fresh[layer, pl.ds(first + 1, 1), :])
            old = recvb[c, :, pl.ds(pl.multiple_of(t * 256 + n * 128, 128), 128)].astype(F32)
            pieces.append(jnp.where(pos_i == where_new, line, old))
        tile = jnp.concatenate(pieces, axis=1).astype(BF16)
        recvb[c, :, at] = tile
        return tile

    def attend(layer):
        ck, cv = 2 * layer, 2 * layer + 1
        a2a_wait(ck)

        def scores(t, _):
            tile = place_new(ck, t, kdup, layer)
            at = pl.ds(pl.multiple_of(t * 16, 16), 16)
            s = nt(qall[layer, at, :], tile) * (head ** -0.5)
            slot, p = iota((16, seq), 0), iota((16, seq), 1)
            limit = jnp.where(slot < 3, len_s[4 * t], jnp.where(slot < 6, len_s[4 * t + 1], jnp.where(slot < 9, len_s[4 * t + 2], len_s[4 * t + 3])))
            sc[at, :] = jnp.where(p <= limit, s, -1e30)
            return 0
        lax.fori_loop(0, groups, scores, 0)
        s = sc[...]
        e = jnp.exp(s - jnp.max(s, axis=-1, keepdims=True))
        sc[...] = e / jnp.sum(e, axis=-1, keepdims=True)
        a2a_wait(cv)

        def values(t, _):
            tile = place_new(cv, t, vdup, layer)
            at = pl.ds(pl.multiple_of(t * 16, 16), 16)
            ov[at, :] = nn(sc[at, :].astype(BF16), tile)
            return 0
        lax.fori_loop(0, groups, values, 0)
        slot2, lane2 = lax.rem(iota((128, 256), 0), 16), iota((128, 256), 1)
        kept = jnp.where(slot2 // 3 == lane2 // 64, ov[...], 0.0)
        both = (kept[:, :128] + kept[:, 128:]).astype(BF16)
        i, j = iota((rows, 128), 0), iota((rows, 128), 1)
        per_head = []
        for r in range(3):
            pick = j == i // 4 * 16 + lax.rem(i, 4) * 3 + r
            got = nn(pick.astype(BF16), both)
            per_head.append(got + pltpu.roll(got, 64, 1))
        return jnp.where(left, per_head[0], per_head[1]).astype(BF16), per_head[2].astype(BF16)[:, :head]

    outs = (ok1, ov1, ok2, ov2)

    def out_copy(c):
        return pltpu.make_async_copy(outst.at[c % 2], outs[c], sem_out.at[c])

    def write_out(c):
        def body(t, _):
            tile = recvb[c, :, pl.ds(pl.multiple_of(t * 256, 256), 256)]
            outst[c % 2, pl.ds(pl.multiple_of(t * 256, 256), 256), :] = tile.T
            return 0
        if c >= 2:
            out_copy(c - 2).wait()
        lax.fori_loop(0, groups, body, 0)
        out_copy(c).start()

    def cols(which):
        return pl.ds(pl.multiple_of(which * half, half), half)

    def all_reduce(r, product, residual, between):
        part[r] = product(1 - core).astype(BF16)
        swap = rcopy(part.at[r], d1.at[r], ss_r.at[r, 0], rs_r.at[r, 0], partner)
        swap.start()
        mine = product(core)
        swap.wait_recv()
        shot[r, chip] = (mine + d1[r].astype(F32)).astype(BF16)
        copies = [swap]
        for n, dx in enumerate((2, 1, 3)):
            copy = rcopy(shot.at[r, chip], shot.at[r, chip], ss_r.at[r, 1 + n], rs_r.at[r, 1 + n], device(dx, 0))
            copy.start()
            copies.append(copy)
        between()
        for n, dx in enumerate((2, 1, 3)):
            origin = lax.rem(chip + CHIPS - dx, CHIPS)
            rcopy(shot.at[r, origin], shot.at[r, origin], ss_r.at[r, 1 + n], rs_r.at[r, 1 + n], device(dx, 0)).wait_recv()
        total = (shot[r, 0].astype(F32) + shot[r, 1].astype(F32)) + (shot[r, 2].astype(F32) + shot[r, 3].astype(F32))
        fin[r, core] = (residual.astype(F32) + total).astype(BF16)
        last = rcopy(fin.at[r, core], fin.at[r, core], ss_r.at[r, 4], rs_r.at[r, 4], partner)
        last.start()
        copies.append(last)
        rcopy(fin.at[r, 1 - core], fin.at[r, 1 - core], ss_r.at[r, 4], rs_r.at[r, 4], partner).wait_recv()
        return copies, jnp.concatenate([fin[r, 0], fin[r, 1]], axis=1).astype(F32)

    def gates(layer, m):
        logits = nt(wr[layer], m)
        e_i = iota((experts, rows), 0)
        chosen = e_i == choice[layer, 0:1, :]
        for n in range(1, choice.shape[1]):
            chosen = chosen | (e_i == choice[layer, n:n + 1, :])
        top = jnp.max(jnp.where(chosen, logits, -3e38), axis=0, keepdims=True)
        weight = jnp.where(chosen, jnp.exp(jnp.where(chosen, logits - top, 0.0)), 0.0)
        gate = (weight / jnp.sum(weight, axis=0, keepdims=True)).T
        for n in range(experts // 2):
            pair = jnp.where(left, gate[:, 2 * n:2 * n + 1], gate[:, 2 * n + 1:2 * n + 2])
            gexp[n // 2, :, (n % 2) * 128:(n % 2 + 1) * 128] = pair

    def experts_up(layer, m):
        def body(c, _):
            w_copy(layer, 0, c).wait()
            w_copy(layer, 1, c).wait()
            at = pl.ds(pl.multiple_of(c * step, step), step)
            g = nt(m, wg[layer, at, :])
            up = nt(m, wu[layer, at, :])
            ubuf[layer, :, at] = (jax.nn.silu(g) * up * gexp[c]).astype(BF16)
            return 0
        lax.fori_loop(0, CHUNKS, body, 0)

        def wait_down(c, _):
            w_copy(layer, 2, c).wait()
            return 0
        lax.fori_loop(0, CHUNKS, wait_down, 0)

    for copy in small:
        copy.wait()
    x = hid[...].astype(F32)
    project(0, x)
    loads[2].wait()
    permute(2)
    loads[3].wait()
    permute(3)
    keep_own(2)
    keep_own(3)

    pending = []
    for layer in range(2):
        if layer:
            project(layer, x)
        first, second = attend(layer)
        n1 = first.shape[1]

        def out_product(which, layer=layer, first=first, second=second, n1=n1):
            return nn(first, wo[layer, :n1, cols(which)]) + nn(second, wo[layer, n1:, cols(which)])

        def between_attn(layer=layer):
            if layer == 0:
                for c in (2, 3):
                    for n in range(7):
                        a2a_copy(c, n).start()
            write_out(2 * layer)
            write_out(2 * layer + 1)

        residual = fin[2 * layer - 1, core] if layer else hid[:, cols(core)]
        copies, x = all_reduce(2 * layer, out_product, residual, between_attn)
        pending += copies
        m = norm(x, gm[layer:layer + 1, :])
        gates(layer, m)
        experts_up(layer, m)

        def down_product(which, layer=layer):
            return nn(ubuf[layer], wd[layer, :, cols(which)])

        copies, x = all_reduce(2 * layer + 1, down_product, fin[2 * layer, core], lambda: None)
        pending += copies
    out_hid[...] = x.astype(BF16)

    for copy in pending:
        copy.wait_send()
    for c in range(4):
        for n in range(7):
            a2a_copy(c, n).wait_send()
        if c >= 2:
            out_copy(c).wait()


def solution(mesh):
    seq_spec = P('dp', 'tp', None, None)
    head_spec = P('dp', None, 'tp', None)
    col_spec = P(None, None, 'tp')
    ff_spec = P(None, None, None, 'tp')
    peers = mesh.shape['tp']

    def local_step(hidden, lengths, choice, keys_one, vals_one, keys_two, vals_two, g_attn, w_q, w_k, w_v, w_o, g_mlp, w_router, w_gate, w_up, w_down):
        rows, pos, heads, head = keys_one.shape
        dim = hidden.shape[1]
        layers, experts, ff = w_down.shape[:3]
        seq = pos * peers
        flat = lambda t: t.reshape(rows * pos * heads, head)
        turn = lambda t: jnp.swapaxes(t, -1, -2)
        wide = experts * ff
        any_spec = pl.BlockSpec(memory_space=pl.ANY)
        cache_shape = jax.ShapeDtypeStruct((rows * head, seq), BF16)
        wqkv_rows = w_q.shape[2] + w_k.shape[2] + 2 * w_v.shape[2]
        scratch = [
            pltpu.VMEM((rows, dim), BF16), pltpu.VMEM((layers, choice.shape[2], rows), jnp.int32),
            pltpu.VMEM((layers, dim), BF16), pltpu.VMEM((layers, dim), BF16),
            pltpu.VMEM((3, rows * pos * heads, head), BF16), pltpu.VMEM((4, heads, pos, rows * head), BF16),
            pltpu.VMEM((4, seq, rows * head), BF16), pltpu.VMEM((2, rows * head, seq), BF16),
            pltpu.VMEM((layers, wqkv_rows, dim), BF16), pltpu.VMEM((layers, w_o.shape[1], dim), BF16),
            pltpu.VMEM((layers, experts, dim), BF16),
            pltpu.VMEM((layers, wide, dim), BF16), pltpu.VMEM((layers, wide, dim), BF16), pltpu.VMEM((layers, wide, dim), BF16),
            pltpu.VMEM((layers, 128, 256), BF16), pltpu.VMEM((layers, rows, 128), F32), pltpu.VMEM((layers, rows, 128), F32),
            pltpu.VMEM((128, seq), F32), pltpu.VMEM((128, 256), F32),
            pltpu.VMEM((CHUNKS, rows, wide // CHUNKS), F32), pltpu.VMEM((layers, rows, wide), BF16),
            pltpu.VMEM((4, rows, dim // 2), BF16), pltpu.VMEM((4, rows, dim // 2), BF16),
            pltpu.VMEM((4, CHIPS, rows, dim // 2), BF16), pltpu.VMEM((4, 2, rows, dim // 2), BF16),
            pltpu.SemaphoreType.DMA((6,)), pltpu.SemaphoreType.DMA((4,)), pltpu.SemaphoreType.DMA((layers, 3, CHUNKS)),
            pltpu.SemaphoreType.DMA((layers, 4)), pltpu.SemaphoreType.DMA((4,)),
            pltpu.SemaphoreType.DMA((4, 7)), pltpu.SemaphoreType.DMA((4, 7)),
            pltpu.SemaphoreType.DMA((4, 5)), pltpu.SemaphoreType.DMA((4, 5)),
        ]
        out = pl.pallas_call(
            kernel,
            name="decode_step",
            out_shape=(jax.ShapeDtypeStruct((rows, dim), BF16),) + (cache_shape,) * 4,
            in_specs=[pl.BlockSpec(memory_space=pltpu.SMEM)] + [any_spec] * 16,
            out_specs=(pl.BlockSpec(memory_space=pltpu.VMEM),) + (any_spec,) * 4,
            scratch_shapes=scratch,
            compiler_params=pltpu.CompilerParams(collective_id=0, has_side_effects=True, vmem_limit_bytes=67043328),
        )(lengths, hidden, turn(choice), flat(keys_one), flat(vals_one), flat(keys_two), flat(vals_two), g_attn, turn(w_q), turn(w_k), turn(w_v), w_o,
          g_mlp, turn(w_router), turn(w_gate).reshape(layers, wide, dim), turn(w_up).reshape(layers, wide, dim), w_down.reshape(layers, wide, dim))
        caches = [jnp.transpose(t.reshape(rows, head, seq), (0, 2, 1))[:, :, None, :] for t in out[1:]]
        return (out[0], *caches)

    return jax.shard_map(local_step, mesh=mesh, in_specs=(P('dp', None), P('dp'), P(None, 'dp', None), seq_spec, seq_spec, seq_spec, seq_spec, P(), col_spec, col_spec, col_spec, P(None, 'tp', None), P(), P(), ff_spec, ff_spec, P(None, None, 'tp', None)), out_specs=(P('dp', None), head_spec, head_spec, head_spec, head_spec), check_vma=False)
```

```python
import functools

import jax
import jax.numpy as jnp
from jax import lax
from jax.experimental import pallas as pl
from jax.experimental.pallas import tpu as pltpu
from jax.sharding import PartitionSpec as P

EPS = 1e-5
THETA = 1000000.0
MESH = pl.DeviceIdType.MESH
F32 = jnp.float32
BF16 = jnp.bfloat16
CHIPS = 4
OFFSETS = ((2, 0), (2, 1), (1, 0), (3, 0), (1, 1), (3, 1), (0, 1))
CHUNKS = 10


def nt(lhs, rhs):
    return lax.dot_general(lhs, rhs, (((1,), (1,)), ((), ())), preferred_element_type=F32)


def nn(lhs, rhs):
    return jnp.dot(lhs, rhs, preferred_element_type=F32)


def iota(shape, dim):
    return lax.broadcasted_iota(jnp.int32, shape, dim)


def kernel(len_s, hid_h, choice_h, k1_h, v1_h, k2_h, v2_h, ga_h, wq_h, wk_h, wv_h, wo_h, gm_h, wr_h, wg_h, wu_h, wd_h,
           out_hid, ok1, ov1, ok2, ov2,
           hid, choice, ga, gm, xst, sendb, recvb, outst, wqkv, wo, wr, wg, wu, wd,
           qall, kdup, vdup, sc, ov, ubuf, part, d1, shot, fin,
           sem_small, sem_x, sem_w, sem_wqkv, sem_out, ss_a, rs_a, ss_r, rs_r):
    rows, dim = hid.shape
    half = dim // 2
    seq = recvb.shape[1]
    pos = seq // (2 * CHIPS)
    lanes = recvb.shape[2]
    groups = lanes // 256
    head = 64
    experts = wr.shape[1]
    step = wg.shape[1] // CHUNKS

    me = lax.axis_index("tp")
    chip, core = me // 2, lax.rem(me, 2)
    partner = chip * 2 + 1 - core

    def device(dx, flip):
        return lax.rem(chip + dx, CHIPS) * 2 + (1 - core if flip else core)

    def rcopy(src, dst, ssem, rsem, peer):
        return pltpu.make_async_remote_copy(src, dst, ssem, rsem, device_id={"tp": peer}, device_id_type=MESH)

    loads = [pltpu.make_async_copy(src, xst.at[c], sem_x.at[c]) for c, src in enumerate((k1_h, v1_h, k2_h, v2_h))]
    small = [pltpu.make_async_copy(src, dst, sem_small.at[n]) for n, (src, dst) in enumerate(
        ((hid_h, hid), (choice_h, choice), (ga_h, ga), (gm_h, gm), (wr_h, wr), (wo_h, wo)))]

    def qkv_loads(layer):
        nq, nk = wq_h.shape[1], wk_h.shape[1]
        return [pltpu.make_async_copy(src.at[layer], wqkv.at[layer, pl.ds(at, size)], sem_wqkv.at[layer, n])
                for n, (src, at, size) in enumerate(((wq_h, 0, nq), (wk_h, nq, nk), (wv_h, nq + nk, nk), (wv_h, nq + 2 * nk, nk)))]

    loads[0].start()
    barrier = pltpu.get_barrier_semaphore()
    for dx, flip in OFFSETS:
        pl.semaphore_signal(barrier, inc=1, device_id={"tp": device(dx, flip)}, device_id_type=MESH)
    for copy in small[:4]:
        copy.start()
    for copy in qkv_loads(0):
        copy.start()
    loads[1].start()
    loads[2].start()
    loads[3].start()
    for copy in small[4:]:
        copy.start()
    for copy in qkv_loads(1):
        copy.start()

    def w_copy(layer, which, c):
        src, dst = ((wg_h, wg), (wu_h, wu), (wd_h, wd))[which]
        at = pl.ds(pl.multiple_of(c * step, step), step)
        return pltpu.make_async_copy(src.at[layer, at], dst.at[layer, at], sem_w.at[layer, which, c])

    def permute(c):
        i, j = iota((128, 128), 0), iota((128, 128), 1)
        perm = (j == lax.rem(i, 16) * 8 + i // 16).astype(BF16)

        for t in range(groups):
            tiles = [xst[c, slice(t * 512 + n * 128, t * 512 + n * 128 + 128), :] for n in range(4)]
            moved = nn(perm, jnp.concatenate(tiles, axis=1)).astype(BF16)
            sendb[c, :, :, slice(t * 256, t * 256 + 256)] = moved.reshape(8, pos, 256)

    def a2a_copy(c, n):
        peer = device(*OFFSETS[n])
        return rcopy(sendb.at[c, peer], recvb.at[c, pl.ds(pl.multiple_of(me * pos, pos), pos)], ss_a.at[c, n], rs_a.at[c, n], peer)

    def a2a_wait(c):
        for n, (dx, flip) in reversed(list(enumerate(OFFSETS))):
            origin = device(CHIPS - dx, flip)
            rcopy(sendb.at[c, origin], recvb.at[c, pl.ds(pl.multiple_of(origin * pos, pos), pos)], ss_a.at[c, n], rs_a.at[c, n], origin).wait_recv()

    def keep_own(c):
        recvb[c, pl.ds(pl.multiple_of(me * pos, pos), pos), :] = sendb[c, me]

    with jax.named_scope("x0_wait"):
        loads[0].wait()
    for layer in range(2):
        def start_weights(c, _, layer=layer):
            w_copy(layer, 0, c).start()
            w_copy(layer, 1, c).start()
            w_copy(layer, 2, c).start()
            return 0
        lax.fori_loop(0, CHUNKS, start_weights, 0)

    with jax.named_scope("permute0"):
        permute(0)
    with jax.named_scope("barrier"):
        pl.semaphore_wait(barrier, len(OFFSETS))
    for n in range(7):
        a2a_copy(0, n).start()
    with jax.named_scope("permute1"):
        loads[1].wait()
        permute(1)
    for n in range(7):
        a2a_copy(1, n).start()
    keep_own(0)
    keep_own(1)

    lane = iota((rows, 128), 1)
    row = iota((rows, 128), 0)
    len_f = jnp.zeros((rows, 128), F32)
    for b in range(rows):
        len_f = jnp.where(row == b, len_s[b].astype(F32), len_f)
    freq = jnp.exp(lax.rem(lane, 32).astype(F32) * (-2.0 / head * 13.815510557964274))
    angle = len_f * freq
    cos_t, sin_t = jnp.cos(angle), jnp.sin(angle)
    low = lax.rem(lane, head) < head // 2
    left = lane < head

    def rope(x):
        turned = jnp.where(low, -pltpu.roll(x, 96, 1), pltpu.roll(x, 32, 1))
        return (x * cos_t + turned * sin_t).astype(BF16).astype(F32)

    def norm(x, gain):
        scale = lax.rsqrt(jnp.mean(x * x, axis=-1, keepdims=True) + EPS)
        return (x * scale * gain.astype(F32)).astype(BF16)

    def project(layer, x):
        for copy in qkv_loads(layer):
            copy.wait()
        qkv = nt(norm(x, ga[layer:layer + 1, :]), wqkv[layer])
        t0, t1 = rope(qkv[:, :128]), rope(qkv[:, 128:256])
        s0, s1 = pltpu.roll(t0, 64, 1), pltpu.roll(t1, 64, 1)
        q3 = jnp.concatenate([jnp.where(left, t0, s0), jnp.where(left, s0, t0), jnp.where(left, t1, s1)], axis=0).astype(BF16)
        kdup[layer] = jnp.where(left, s1, t1)
        vdup[layer] = qkv[:, 256:384].astype(BF16).astype(F32)
        i, j = iota((128, 96), 0), iota((128, 96), 1)
        slot = lax.rem(i, 16)
        pick = (slot < 12) & (j == lax.rem(slot, 3) * rows + i // 16 * 4 + slot // 3)
        dup = nn(pick.astype(BF16), q3)
        slot2, lane2 = lax.rem(iota((128, 256), 0), 16), iota((128, 256), 1)
        both = jnp.concatenate([dup, dup], axis=1)
        qall[layer] = jnp.where(slot2 // 3 == lane2 // 64, both, 0.0).astype(BF16)

    def place_new(c, t, fresh, layer):
        at = slice(t * 256, t * 256 + 256)
        pos_i, lane_i = iota((seq, 128), 0), iota((seq, 128), 1)
        pieces = []
        for n in range(2):
            first = t * 4 + 2 * n
            where_new = jnp.where(lane_i < head, len_s[first], len_s[first + 1])
            line = jnp.where(lane_i[:1] < head, fresh[layer, first:first + 1, :], fresh[layer, first + 1:first + 2, :])
            old = recvb[c, :, slice(t * 256 + n * 128, t * 256 + n * 128 + 128)].astype(F32)
            pieces.append(jnp.where(pos_i == where_new, line, old))
        tile = jnp.concatenate(pieces, axis=1).astype(BF16)
        recvb[c, :, at] = tile
        return tile

    def attend(layer):
        ck, cv = 2 * layer, 2 * layer + 1
        with jax.named_scope("wait_keys"):
            a2a_wait(ck)

        def scores(t):
            tile = place_new(ck, t, kdup, layer)
            at = slice(t * 16, t * 16 + 16)
            s = nt(qall[layer, at, :], tile) * (head ** -0.5)
            slot, p = iota((16, seq), 0), iota((16, seq), 1)
            limit = jnp.where(slot < 3, len_s[4 * t], jnp.where(slot < 6, len_s[4 * t + 1], jnp.where(slot < 9, len_s[4 * t + 2], len_s[4 * t + 3])))
            sc[at, :] = jnp.where(p <= limit, s, -1e30)
        with jax.named_scope("scores"):
            for t in range(groups):
                scores(t)
        s = sc[...]
        e = jnp.exp(s - jnp.max(s, axis=-1, keepdims=True))
        sc[...] = e / jnp.sum(e, axis=-1, keepdims=True)
        with jax.named_scope("wait_values"):
            a2a_wait(cv)

        def values(t):
            tile = place_new(cv, t, vdup, layer)
            at = slice(t * 16, t * 16 + 16)
            ov[at, :] = nn(sc[at, :].astype(BF16), tile)
        with jax.named_scope("values"):
            for t in range(groups):
                values(t)
        slot2, lane2 = lax.rem(iota((128, 256), 0), 16), iota((128, 256), 1)
        kept = jnp.where(slot2 // 3 == lane2 // 64, ov[...], 0.0)
        both = (kept[:, :128] + kept[:, 128:]).astype(BF16)
        i, j = iota((rows, 128), 0), iota((rows, 128), 1)
        per_head = []
        for r in range(3):
            pick = j == i // 4 * 16 + lax.rem(i, 4) * 3 + r
            got = nn(pick.astype(BF16), both)
            per_head.append(got + pltpu.roll(got, 64, 1))
        return jnp.where(left, per_head[0], per_head[1]).astype(BF16), per_head[2].astype(BF16)[:, :head]

    outs = (ok1, ov1, ok2, ov2)

    def out_copy(c):
        return pltpu.make_async_copy(outst.at[c % 2], outs[c], sem_out.at[c])

    def write_out(c):
        if c >= 2:
            out_copy(c - 2).wait()
        for t in range(groups):
            outst[c % 2, t * 256:(t + 1) * 256, :] = recvb[c, :, t * 256:(t + 1) * 256].T
        out_copy(c).start()

    def cols(which):
        return pl.ds(pl.multiple_of(which * half, half), half)

    def block(which, q, size):
        return pl.ds(pl.multiple_of(which * half + q * size, size), size)

    def all_reduce(r, product, residual, between, parts):
        size = half // parts
        per = shot.shape[2] // parts
        copies = []

        def send(src, dst, kind, q, peer):
            copy = rcopy(src, dst, ss_r.at[r, kind, q], rs_r.at[r, kind, q], peer)
            copy.start()
            copies.append(copy)
            return copy

        def put(ref, q, value):
            for n in range(per):
                ref[q * per + n] = value[:, n * (size // per):(n + 1) * (size // per)].astype(BF16)

        def get(ref, q):
            return jnp.concatenate([ref[q * per + n].astype(F32) for n in range(per)], axis=1)

        swaps = []
        for q in range(parts):
            put(part.at[r], q, product(1 - core, q, size))
            at = pl.ds(q * per, per)
            swaps.append(send(part.at[r, at], d1.at[r, at], 0, q, partner))
        for q in range(parts):
            mine = product(core, q, size)
            with jax.named_scope("swap_wait"):
                swaps[q].wait_recv()
            put(shot.at[r, chip], q, mine + get(d1.at[r], q))
            piece = shot.at[r, chip, pl.ds(q * per, per)]
            for n, dx in enumerate((2, 1, 3)):
                send(piece, piece, 1 + n, q, device(dx, 0))
        with jax.named_scope("between"):
            between()
        for q in range(parts):
            at = pl.ds(q * per, per)
            with jax.named_scope("shot_wait"):
                for n, dx in enumerate((2, 1, 3)):
                    piece = shot.at[r, lax.rem(chip + CHIPS - dx, CHIPS), at]
                    rcopy(piece, piece, ss_r.at[r, 1 + n, q], rs_r.at[r, 1 + n, q], device(dx, 0)).wait_recv()
            total = (get(shot.at[r, 0], q) + get(shot.at[r, 1], q)) + (get(shot.at[r, 2], q) + get(shot.at[r, 3], q))
            put(fin.at[r, core], q, residual(q, size) + total)
            send(fin.at[r, core, at], fin.at[r, core, at], 4, q, partner)
        with jax.named_scope("last_wait"):
            for q in range(parts):
                piece = fin.at[r, 1 - core, pl.ds(q * per, per)]
                rcopy(piece, piece, ss_r.at[r, 4, q], rs_r.at[r, 4, q], partner).wait_recv()
        pieces = [fin[r, h, n].astype(F32) for h in range(2) for n in range(shot.shape[2])]
        return copies, jnp.concatenate(pieces, axis=1)

    def gates(layer, m):
        logits = nt(wr[layer], m)
        e_i = iota((experts, rows), 0)
        chosen = e_i == choice[layer, 0:1, :]
        for n in range(1, choice.shape[1]):
            chosen = chosen | (e_i == choice[layer, n:n + 1, :])
        top = jnp.max(jnp.where(chosen, logits, -3e38), axis=0, keepdims=True)
        weight = jnp.where(chosen, jnp.exp(jnp.where(chosen, logits - top, 0.0)), 0.0)
        return (weight / jnp.sum(weight, axis=0, keepdims=True)).T

    def wait_weights(layer):
        def body(c, _):
            for which in range(3):
                w_copy(layer, which, c).wait()
            return 0
        lax.fori_loop(0, CHUNKS, body, 0)

    def experts_up(layer, m):
        gate = gates(layer, m)
        pairs = step // 128
        for c in range(CHUNKS):
            at = slice(c * step, (c + 1) * step)
            g = nt(m, wg[layer, at, :])
            up = nt(m, wu[layer, at, :])
            wide = jnp.concatenate([jnp.where(left, gate[:, 2 * n:2 * n + 1], gate[:, 2 * n + 1:2 * n + 2]) for n in range(c * pairs, (c + 1) * pairs)], axis=1)
            ubuf[layer, :, at] = (jax.nn.silu(g) * up * wide).astype(BF16)

    for copy in small:
        copy.wait()
    x = hid[...].astype(F32)
    with jax.named_scope("project"):
        project(0, x)
    with jax.named_scope("permute23"):
        loads[2].wait()
        permute(2)
        loads[3].wait()
        permute(3)
        keep_own(2)
        keep_own(3)

    pending = []
    for layer in range(2):
        if layer:
            with jax.named_scope("project"):
                project(layer, x)
        first, second = attend(layer)
        n1 = first.shape[1]

        def out_product(which, q, size, layer=layer, first=first, second=second, n1=n1):
            at = block(which, q, size)
            return nn(first, wo[layer, :n1, at]) + nn(second, wo[layer, n1:, at])

        def between_attn(layer=layer):
            if layer == 0:
                for c in (2, 3):
                    for n in range(7):
                        a2a_copy(c, n).start()
            write_out(2 * layer)
            write_out(2 * layer + 1)
            wait_weights(layer)

        def residual_attn(q, size, layer=layer):
            if layer:
                return jnp.concatenate([fin[2 * layer - 1, core, n].astype(F32) for n in range(shot.shape[2])], axis=1)
            return hid[:, block(core, q, size)].astype(F32)

        copies, x = all_reduce(2 * layer, out_product, residual_attn, between_attn, 1)
        pending += copies
        m = norm(x, gm[layer:layer + 1, :])
        with jax.named_scope("up"):
            experts_up(layer, m)

        def down_product(which, q, size, layer=layer):
            with jax.named_scope("down"):
                return nn(ubuf[layer], wd[layer, :, block(which, q, size)])

        def residual_moe(q, size, layer=layer):
            return fin[2 * layer, core, q].astype(F32)

        copies, x = all_reduce(2 * layer + 1, down_product, residual_moe, lambda: None, 2)
        pending += copies
    out_hid[...] = x.astype(BF16)

    with jax.named_scope("tail"):
        for copy in pending:
            copy.wait_send()
        for c in range(4):
            for n in range(7):
                a2a_copy(c, n).wait_send()
            if c >= 2:
                out_copy(c).wait()


def finish(*refs):
    n = (len(refs) - 2) // 3
    srcs, dsts, bufs, in_sem, out_sem = refs[:n], refs[n:2 * n], refs[2 * n:3 * n], refs[-2], refs[-1]
    into = [pltpu.make_async_copy(srcs[i], bufs[i], in_sem.at[i]) for i in range(n)]
    out = [pltpu.make_async_copy(bufs[i], dsts[i], out_sem.at[i]) for i in range(n)]
    for copy in into:
        copy.start()
    for i in range(n):
        into[i].wait()
        out[i].start()
    for copy in out:
        copy.wait()


def solution(mesh):
    seq_spec = P('dp', 'tp', None, None)
    head_spec = P('dp', None, 'tp', None)
    col_spec = P(None, None, 'tp')
    ff_spec = P(None, None, None, 'tp')
    peers = mesh.shape['tp']

    def local_step(hidden, lengths, choice, keys_one, vals_one, keys_two, vals_two, g_attn, w_q, w_k, w_v, w_o, g_mlp, w_router, w_gate, w_up, w_down):
        rows, pos, heads, head = keys_one.shape
        dim = hidden.shape[1]
        layers, experts, ff = w_down.shape[:3]
        seq = pos * peers
        flat = lambda t: t.reshape(rows * pos * heads, head)
        turn = lambda t: jnp.swapaxes(t, -1, -2)
        wide = experts * ff
        any_spec = pl.BlockSpec(memory_space=pl.ANY)
        cache_shape = jax.ShapeDtypeStruct((rows * head, seq), BF16)
        wqkv_rows = w_q.shape[2] + w_k.shape[2] + 2 * w_v.shape[2]
        scratch = [
            pltpu.VMEM((rows, dim), BF16), pltpu.VMEM((layers, choice.shape[2], rows), jnp.int32),
            pltpu.VMEM((layers, dim), BF16), pltpu.VMEM((layers, dim), BF16),
            pltpu.VMEM((4, rows * pos * heads, head), BF16), pltpu.VMEM((4, heads, pos, rows * head), BF16),
            pltpu.VMEM((4, seq, rows * head), BF16), pltpu.VMEM((2, rows * head, seq), BF16),
            pltpu.VMEM((layers, wqkv_rows, dim), BF16), pltpu.VMEM((layers, w_o.shape[1], dim), BF16),
            pltpu.VMEM((layers, experts, dim), BF16),
            pltpu.VMEM((layers, wide, dim), BF16), pltpu.VMEM((layers, wide, dim), BF16), pltpu.VMEM((layers, wide, dim), BF16),
            pltpu.VMEM((layers, 128, 256), BF16), pltpu.VMEM((layers, rows, 128), F32), pltpu.VMEM((layers, rows, 128), F32),
            pltpu.VMEM((128, seq), F32), pltpu.VMEM((128, 256), F32),
            pltpu.VMEM((layers, rows, wide), BF16),
            pltpu.VMEM((4, 2, rows, dim // 4), BF16), pltpu.VMEM((4, 2, rows, dim // 4), BF16),
            pltpu.VMEM((4, CHIPS, 2, rows, dim // 4), BF16), pltpu.VMEM((4, 2, 2, rows, dim // 4), BF16),
            pltpu.SemaphoreType.DMA((6,)), pltpu.SemaphoreType.DMA((4,)), pltpu.SemaphoreType.DMA((layers, 3, CHUNKS)),
            pltpu.SemaphoreType.DMA((layers, 4)), pltpu.SemaphoreType.DMA((4,)),
            pltpu.SemaphoreType.DMA((4, 7)), pltpu.SemaphoreType.DMA((4, 7)),
            pltpu.SemaphoreType.DMA((4, 5, 2)), pltpu.SemaphoreType.DMA((4, 5, 2)),
        ]
        out = pl.pallas_call(
            kernel,
            name="decode_step",
            out_shape=(jax.ShapeDtypeStruct((rows, dim), BF16),) + (cache_shape,) * 4,
            in_specs=[pl.BlockSpec(memory_space=pltpu.SMEM)] + [any_spec] * 16,
            out_specs=(pl.BlockSpec(memory_space=pltpu.VMEM),) + (any_spec,) * 4,
            scratch_shapes=scratch,
            compiler_params=pltpu.CompilerParams(collective_id=0, has_side_effects=True, vmem_limit_bytes=67043328),
        )(lengths, hidden, turn(choice), flat(keys_one), flat(vals_one), flat(keys_two), flat(vals_two), g_attn, turn(w_q), turn(w_k), turn(w_v), w_o,
          g_mlp, turn(w_router), turn(w_gate).reshape(layers, wide, dim), turn(w_up).reshape(layers, wide, dim), w_down.reshape(layers, wide, dim))
        out = pl.pallas_call(
            finish,
            name="finish",
            out_shape=[jax.ShapeDtypeStruct(t.shape, t.dtype) for t in out],
            in_specs=[any_spec] * len(out),
            out_specs=[any_spec] * len(out),
            scratch_shapes=[pltpu.VMEM(t.shape, t.dtype) for t in out] + [pltpu.SemaphoreType.DMA((len(out),))] * 2,
        )(*out)
        caches = [jnp.transpose(t.reshape(rows, head, seq), (0, 2, 1))[:, :, None, :] for t in out[1:]]
        return (out[0], *caches)

    return jax.shard_map(local_step, mesh=mesh, in_specs=(P('dp', None), P('dp'), P(None, 'dp', None), seq_spec, seq_spec, seq_spec, seq_spec, P(), col_spec, col_spec, col_spec, P(None, 'tp', None), P(), P(), ff_spec, ff_spec, P(None, None, 'tp', None)), out_specs=(P('dp', None), head_spec, head_spec, head_spec, head_spec), check_vma=False)
```

```python
import functools

import jax
import jax.numpy as jnp
from jax import lax
from jax.experimental import pallas as pl
from jax.experimental.pallas import tpu as pltpu
from jax.sharding import PartitionSpec as P

EPS = 1e-5
THETA = 1000000.0
MESH = pl.DeviceIdType.MESH
F32 = jnp.float32
BF16 = jnp.bfloat16
LANES, WIDE, TILE, HEAD = 128, 256, 16, 64
CHIPS = 4
OFFSETS = ((2, 0), (2, 1), (1, 0), (3, 0), (1, 1), (3, 1), (0, 1))
def units(cache, *which):
    pairs = ((0,), (1,), (2, 3), (4, 5), (6,))
    return [(cache, n) for k in which for n in pairs[k]]


WINDOWS = (
    units(2, 2),
    units(2, 4, 0) + units(3, 4),
    [],
    units(2, 1),
    units(2, 3) + units(3, 0, 1, 2, 3),
    units(0, 4, 0, 1, 2) + units(1, 4),
    units(0, 3) + units(1, 0, 1, 2, 3),
)
CHUNKS = 10


def nt(lhs, rhs):
    return lax.dot_general(lhs, rhs, (((1,), (1,)), ((), ())), preferred_element_type=F32)


def nn(lhs, rhs):
    return jnp.dot(lhs, rhs, preferred_element_type=F32)


def iota(shape, dim):
    return lax.broadcasted_iota(jnp.int32, shape, dim)


def kernel(len_h, hid_h, choice_h, k1_h, v1_h, k2_h, v2_h, ga_h, wq_h, wk_h, wv_h, wo_h, gm_h, wr_h, wg_h, wu_h, wd_h,
           out_hid, ok1, ov1, ok2, ov2,
           len_s, hid, choice, ga, gm, xst, sendb, recvb, wqkv, wo, wr, wg, wu, wd,
           qall, kdup, vdup, sc, ov, ubuf, part, d1, shot, fin, qrecv, psend, precv,
           sem_small, sem_x, sem_w, sem_wqkv, ss_a, rs_a, ss_r, rs_r, ss_q, rs_q, ss_p, rs_p):
    rows, dim = hid.shape
    half = dim // 2
    seq = recvb.shape[1]
    pos = seq // (2 * CHIPS)
    lanes = recvb.shape[2]
    groups = lanes // WIDE
    head = HEAD
    experts = wr.shape[1]
    step = wg.shape[1] // CHUNKS

    me = lax.axis_index("tp")
    chip, core = me // 2, lax.rem(me, 2)
    partner = chip * 2 + 1 - core

    def device(dx, flip):
        return lax.rem(chip + dx, CHIPS) * 2 + (1 - core if flip else core)

    def rcopy(src, dst, ssem, rsem, peer):
        return pltpu.make_async_remote_copy(src, dst, ssem, rsem, device_id={"tp": peer}, device_id_type=MESH)

    def drain(ref, sem):
        pltpu.make_async_copy(ref, ref, sem).wait()

    loads = [pltpu.make_async_copy(src, xst.at[c], sem_x.at[c]) for c, src in enumerate((k1_h, v1_h, k2_h, v2_h))]
    small = [pltpu.make_async_copy(src, dst, sem_small.at[n]) for n, (src, dst) in enumerate(
        ((hid_h, hid), (len_h, len_s), (ga_h, ga), (gm_h, gm), (choice_h, choice), (wr_h, wr), (wo_h, wo)))]

    def qkv_loads(layer):
        nq, nk = wq_h.shape[1], wk_h.shape[1]
        return [pltpu.make_async_copy(src.at[layer], wqkv.at[layer, pl.ds(at, size)], sem_wqkv.at[layer])
                for src, at, size in ((wq_h, 0, nq), (wk_h, nq, nk), (wv_h, nq + nk, nk), (wv_h, nq + 2 * nk, nk))]

    small[0].start()
    for copy in qkv_loads(0):
        copy.start()
    for copy in small[1:4]:
        copy.start()
    barrier = pltpu.get_barrier_semaphore()
    for dx, flip in OFFSETS:
        pl.semaphore_signal(barrier, inc=1, device_id={"tp": device(dx, flip)}, device_id_type=MESH)
    for c in (2, 0, 1, 3):
        loads[c].start()
    for copy in small[4:]:
        copy.start()
    for copy in qkv_loads(1):
        copy.start()

    def w_copy(layer, which, c):
        src, dst = ((wg_h, wg), (wu_h, wu), (wd_h, wd))[which]
        at = pl.ds(pl.multiple_of(c * step, step), step)
        return pltpu.make_async_copy(src.at[layer, at], dst.at[layer, at], sem_w.at[layer, which])

    def permute(c):
        i, j = iota((LANES, LANES), 0), iota((LANES, LANES), 1)
        perm = (j == lax.rem(i, TILE) * 8 + i // TILE).astype(BF16)

        for t in range(groups):
            tiles = [xst[c, slice(t * 512 + n * LANES, t * 512 + n * LANES + LANES), :] for n in range(4)]
            moved = nn(perm, jnp.concatenate(tiles, axis=1)).astype(BF16)
            sendb[c, :, :, slice(t * WIDE, t * WIDE + WIDE)] = moved.reshape(8, pos, WIDE)

    def a2a_copy(c, n):
        peer = device(*OFFSETS[n])
        return rcopy(sendb.at[c, peer], recvb.at[c, pl.ds(pl.multiple_of(me * pos, pos), pos)], ss_a.at[c], rs_a.at[c], peer)

    def a2a_wait(c):
        drain(recvb.at[c, pl.ds(0, len(OFFSETS) * pos)], rs_a.at[c])

    def keep_own(c):
        recvb[c, pl.ds(pl.multiple_of(me * pos, pos), pos), :] = sendb[c, me]

    for layer in range(2):
        def start_weights(c, _, layer=layer):
            w_copy(layer, 0, c).start()
            w_copy(layer, 1, c).start()
            w_copy(layer, 2, c).start()
            return 0
        lax.fori_loop(0, CHUNKS, start_weights, 0)

    with jax.named_scope("small_wait"):
        for copy in small[:4]:
            copy.wait()
    lane = iota((rows, LANES), 1)
    row = iota((rows, LANES), 0)
    len_f = jnp.zeros((rows, LANES), F32)
    for b in range(rows):
        len_f = jnp.where(row == b, len_s[b].astype(F32), len_f)
    freq = jnp.exp(lax.rem(lane, 32).astype(F32) * (-2.0 / head * 13.815510557964274))
    angle = len_f * freq
    cos_t, sin_t = jnp.cos(angle), jnp.sin(angle)
    low = lax.rem(lane, head) < head // 2
    left = lane < head

    def rope(x):
        turned = jnp.where(low, -pltpu.roll(x, 96, 1), pltpu.roll(x, 32, 1))
        return (x * cos_t + turned * sin_t).astype(BF16).astype(F32)

    def norm(x, gain):
        scale = lax.rsqrt(jnp.mean(x * x, axis=-1, keepdims=True) + EPS)
        return (x * scale * gain.astype(F32)).astype(BF16)

    def project(layer, x):
        drain(wqkv.at[layer], sem_wqkv.at[layer])
        qkv = nt(norm(x, ga[layer:layer + 1, :]), wqkv[layer])
        t0, t1 = rope(qkv[:, :LANES]), rope(qkv[:, LANES:WIDE])
        s0, s1 = pltpu.roll(t0, HEAD, 1), pltpu.roll(t1, HEAD, 1)
        q3 = jnp.concatenate([jnp.where(left, t0, s0), jnp.where(left, s0, t0), jnp.where(left, t1, s1)], axis=0).astype(BF16)
        kdup[layer] = jnp.where(left, s1, t1)
        vdup[layer] = qkv[:, WIDE:384].astype(BF16).astype(F32)
        return q3

    def block_queries(q3):
        i, j = iota((LANES, 96), 0), iota((LANES, 96), 1)
        slot = lax.rem(i, TILE)
        pick = (slot < 12) & (j == lax.rem(slot, 3) * rows + i // TILE * 4 + slot // 3)
        dup = nn(pick.astype(BF16), q3)
        slot2, lane2 = lax.rem(iota((LANES, WIDE), 0), TILE), iota((LANES, WIDE), 1)
        both = jnp.concatenate([dup, dup], axis=1)
        qall[...] = jnp.where(slot2 // 3 == lane2 // HEAD, both, 0.0).astype(BF16)

    hb = rows // 2
    prow, plane = iota((hb * 4, LANES), 0), iota((hb * 4, LANES), 1)
    pleft = plane < head

    def pack(table, cells):
        width = table.shape[0]
        i, j = iota((hb * 4, width), 0), iota((hb * 4, width), 1)
        low_half = nn(cells(i, j, 0).astype(BF16), table)
        high_half = nn(cells(i, j, hb).astype(BF16), table)
        return jnp.where(pleft, low_half, high_half)

    def pack_queries(q3):
        return pack(q3, lambda i, j, b0: (lax.rem(i, 4) < 3) & (j == lax.rem(i, 4) * rows + i // 4 + b0))

    def pack_fresh(table):
        return pack(table.astype(BF16), lambda i, j, b0: j == i // 4 + b0)

    def to_all(n, src, dst, ssem, rsem):
        return rcopy(src, dst, ssem, rsem, device(*OFFSETS[n]))

    def q_copy(n):
        return to_all(n, qrecv.at[me], qrecv.at[me], ss_q, rs_q)

    def p_copy(n):
        return to_all(n, psend.at[device(*OFFSETS[n])], precv.at[me], ss_p, rs_p)

    def seven(ref):
        return ref.at[pl.ds(0, len(OFFSETS))]

    def local_attend():
        row_i, lane_i = iota((LANES, LANES), 0), iota((LANES, LANES), 1)
        wide_row, wide_lane = iota((LANES, WIDE), 0), iota((LANES, WIDE), 1)
        own_head = row_i // TILE == lax.rem(lane_i, 8)
        where_pos = me * pos + lane_i // 8
        in_group = lax.rem(row_i, TILE) // 4
        slot = lax.rem(row_i, 4)
        diagonal = wide_lane // head == lax.rem(wide_row, TILE) // 4
        half_lane = lane_i < head
        lane_in = lax.rem(lane_i, head)
        done = []
        for t in range(groups):
            at = slice(t % 4 * TILE, t % 4 * TILE + TILE)
            q = qrecv[:, at, :].reshape(LANES, LANES).astype(F32)
            q = jnp.where(half_lane if t < 4 else ~half_lane, q, 0.0)
            q = q + pltpu.roll(q, HEAD, 1)
            q = jnp.where(diagonal, jnp.concatenate([q, q], axis=1), 0.0).astype(BF16)
            keys = jnp.concatenate([xst[0, b * LANES:(b + 1) * LANES, :] for b in range(4 * t, 4 * t + 4)], axis=1)
            vals = jnp.concatenate([xst[1, b * LANES:(b + 1) * LANES, :] for b in range(4 * t, 4 * t + 4)], axis=1)
            s = nt(q, keys) * (head ** -0.5)
            limit = jnp.where(in_group == 0, len_s[4 * t], jnp.where(in_group == 1, len_s[4 * t + 1], jnp.where(in_group == 2, len_s[4 * t + 2], len_s[4 * t + 3])))
            valid = own_head & (where_pos < limit)
            s = jnp.where(valid, s, -1e30)
            top = jnp.max(s, axis=-1, keepdims=True)
            p = jnp.where(valid, jnp.exp(s - top), 0.0)
            total = jnp.sum(p, axis=-1, keepdims=True)
            o = jnp.where(diagonal, nn(p.astype(BF16), vals), 0.0)
            o = o[:, :LANES] + o[:, LANES:]
            o = o + pltpu.roll(o, HEAD, 1)
            stat = jnp.where(slot == 3, 0.0, jnp.where(lane_in == slot, top, jnp.where(lane_in == slot + 3, total, 0.0)))
            stat = pltpu.roll(stat, 1, 0) + pltpu.roll(stat, 2, 0) + pltpu.roll(stat, 3, 0)
            done.append(jnp.where(slot == 3, stat, o))
            if t >= 4:
                psend[:, at, :] = jnp.where(half_lane, done[t - 4], done[t]).reshape(8, TILE, LANES)

    def half_sum(x):
        low_half = jnp.sum(jnp.where(pleft, x, 0.0), axis=-1, keepdims=True)
        high_half = jnp.sum(jnp.where(pleft, 0.0, x), axis=-1, keepdims=True)
        return jnp.where(pleft, low_half, high_half)

    def merge(queries, fresh_k, fresh_v):
        slot, lane_in = lax.rem(prow, 4), lax.rem(plane, head)
        n_rows = prow.shape[0]
        parts = []
        for n in range(2 * CHIPS):
            x = precv[n]
            stat = jnp.where(slot == 0, pltpu.roll(x, n_rows - 3, 0), jnp.where(slot == 1, pltpu.roll(x, n_rows - 2, 0), pltpu.roll(x, n_rows - 1, 0)))
            parts.append((half_sum(jnp.where(lane_in == slot, stat, 0.0)), half_sum(jnp.where(lane_in == slot + 3, stat, 0.0)), x))
        own = half_sum(queries * fresh_k) * (head ** -0.5)
        top = own
        for m, _, _ in parts:
            top = jnp.maximum(top, m)
        weight = jnp.exp(own - top)
        den, num = weight, weight * fresh_v
        for m, total, o in parts:
            weight = jnp.exp(m - top)
            den += weight * total
            num += weight * o
        o = jnp.where(slot == 3, 0.0, num / den).astype(BF16)
        i, j = iota((rows, n_rows), 0), iota((rows, n_rows), 1)
        kept = left == (row < hb)
        per_head = []
        for r in range(3):
            got = jnp.where(kept, nn((j == lax.rem(i, hb) * 4 + r).astype(BF16), o), 0.0)
            per_head.append(got + pltpu.roll(got, HEAD, 1))
        return jnp.where(left, per_head[0], per_head[1]).astype(BF16), per_head[2].astype(BF16)[:, :head]

    def place_new(c, t, fresh, layer):
        at = slice(t * WIDE, t * WIDE + WIDE)
        pos_i, lane_i = iota((seq, LANES), 0), iota((seq, LANES), 1)
        pieces = []
        for n in range(2):
            first = t * 4 + 2 * n
            where_new = jnp.where(lane_i < head, len_s[first], len_s[first + 1])
            line = jnp.where(lane_i[:1] < head, fresh[layer, first:first + 1, :], fresh[layer, first + 1:first + 2, :])
            old = recvb[c, :, slice(t * WIDE + n * LANES, t * WIDE + n * LANES + LANES)].astype(F32)
            pieces.append(jnp.where(pos_i == where_new, line, old))
        tile = jnp.concatenate(pieces, axis=1).astype(BF16)
        recvb[c, :, at] = tile
        return tile

    def attend(layer):
        ck, cv = 2 * layer, 2 * layer + 1
        with jax.named_scope("wait_keys"):
            a2a_wait(ck)

        def scores(t):
            tile = place_new(ck, t, kdup, layer)
            at = slice(t * TILE, t * TILE + TILE)
            s = nt(qall[at, :], tile) * (head ** -0.5)
            slot, p = iota((TILE, seq), 0), iota((TILE, seq), 1)
            limit = jnp.where(slot < 3, len_s[4 * t], jnp.where(slot < 6, len_s[4 * t + 1], jnp.where(slot < 9, len_s[4 * t + 2], len_s[4 * t + 3])))
            sc[at, :] = jnp.where(p <= limit, s, -1e30)
        with jax.named_scope("scores"):
            for t in range(groups):
                scores(t)
        s = sc[...]
        e = jnp.exp(s - jnp.max(s, axis=-1, keepdims=True))
        sc[...] = e / jnp.sum(e, axis=-1, keepdims=True)
        with jax.named_scope("wait_values"):
            a2a_wait(cv)

        def values(t):
            tile = place_new(cv, t, vdup, layer)
            at = slice(t * TILE, t * TILE + TILE)
            ov[at, :] = nn(sc[at, :].astype(BF16), tile)
        with jax.named_scope("values"):
            for t in range(groups):
                values(t)
        slot2, lane2 = lax.rem(iota((LANES, WIDE), 0), TILE), iota((LANES, WIDE), 1)
        kept = jnp.where(slot2 // 3 == lane2 // HEAD, ov[...], 0.0)
        both = (kept[:, :LANES] + kept[:, LANES:]).astype(BF16)
        i, j = iota((rows, LANES), 0), iota((rows, LANES), 1)
        per_head = []
        for r in range(3):
            pick = j == i // 4 * TILE + lax.rem(i, 4) * 3 + r
            got = nn(pick.astype(BF16), both)
            per_head.append(got + pltpu.roll(got, HEAD, 1))
        return jnp.where(left, per_head[0], per_head[1]).astype(BF16), per_head[2].astype(BF16)[:, :head]

    outs = (ok1, ov1, ok2, ov2)

    def write_out(c):
        for t in range(groups):
            outs[c][t * WIDE:(t + 1) * WIDE, :] = recvb[c, :, t * WIDE:(t + 1) * WIDE].T

    def cols(which):
        return pl.ds(pl.multiple_of(which * half, half), half)

    def block(which, q, size):
        return pl.ds(pl.multiple_of(which * half + q * size, size), size)

    def all_reduce(r, product, residual, between, parts, window):
        size = half // parts
        per = shot.shape[2] // parts

        def send(ref, dst, ssem, rsem, peer):
            rcopy(ref, dst, ss_r.at[r, ssem], rs_r.at[r, rsem], peer).start()

        def put(ref, q, value):
            for n in range(per):
                ref[q * per + n] = value[:, n * (size // per):(n + 1) * (size // per)].astype(BF16)

        def get(ref, q):
            return jnp.concatenate([ref[q * per + n].astype(F32) for n in range(per)], axis=1)

        for q in range(parts):
            put(part.at[r], q, product(1 - core, q, size))
            at = pl.ds(q * per, per)
            send(part.at[r, at], d1.at[r, at], 0, q, partner)
        for q in range(parts):
            mine = product(core, q, size)
            with jax.named_scope("swap_wait"):
                drain(d1.at[r, pl.ds(q * per, per)], rs_r.at[r, q])
            put(shot.at[r, chip], q, mine + get(d1.at[r], q))
            piece = shot.at[r, chip, pl.ds(q * per, per)]
            for dx in (2, 1, 3):
                send(piece, piece, 1, 2 + q, device(dx, 0))
        with jax.named_scope("between"):
            between()
        for q in range(parts):
            at = pl.ds(q * per, per)
            with jax.named_scope("shot_wait"):
                drain(shot.at[r, pl.ds(0, CHIPS - 1), at], rs_r.at[r, 2 + q])
            total = (get(shot.at[r, 0], q) + get(shot.at[r, 1], q)) + (get(shot.at[r, 2], q) + get(shot.at[r, 3], q))
            put(fin.at[r, core], q, residual(q, size) + total)
            send(fin.at[r, core, at], fin.at[r, core, at], 0, 4, partner)
        send_caches(window)
        with jax.named_scope("last_wait"):
            drain(fin.at[r, 1 - core], rs_r.at[r, 4])
        pieces = [fin[r, h, n].astype(F32) for h in range(2) for n in range(shot.shape[2])]
        return jnp.concatenate(pieces, axis=1)

    def gates(layer, m):
        logits = nt(wr[layer], m)
        e_i = iota((experts, rows), 0)
        chosen = e_i == choice[layer, 0:1, :]
        for n in range(1, choice.shape[1]):
            chosen = chosen | (e_i == choice[layer, n:n + 1, :])
        top = jnp.max(jnp.where(chosen, logits, -3e38), axis=0, keepdims=True)
        weight = jnp.where(chosen, jnp.exp(jnp.where(chosen, logits - top, 0.0)), 0.0)
        return (weight / jnp.sum(weight, axis=0, keepdims=True)).T

    def wait_weights(layer):
        for which, ref in enumerate((wg, wu, wd)):
            drain(ref.at[layer], sem_w.at[layer, which])

    def experts_up(layer, m):
        gate = gates(layer, m)
        pairs = step // LANES
        for c in range(CHUNKS):
            at = slice(c * step, (c + 1) * step)
            g = nt(m, wg[layer, at, :])
            up = nt(m, wu[layer, at, :])
            wide = jnp.concatenate([jnp.where(left, gate[:, 2 * n:2 * n + 1], gate[:, 2 * n + 1:2 * n + 2]) for n in range(c * pairs, (c + 1) * pairs)], axis=1)
            ubuf[:, at] = (jax.nn.silu(g) * up * wide).astype(BF16)

    def send_caches(wanted):
        for c, n in wanted:
            a2a_copy(c, n).start()

    x = hid[...].astype(F32)
    with jax.named_scope("project"):
        q3 = project(0, x)
        queries = pack_queries(q3)
        fresh_k, fresh_v = pack_fresh(kdup[0]), pack_fresh(vdup[0])
        qrecv[me] = queries.astype(BF16)
    with jax.named_scope("barrier"):
        pl.semaphore_wait(barrier, len(OFFSETS))
    for n in range(7):
        q_copy(n).start()
    with jax.named_scope("permute2"):
        loads[2].wait()
        permute(2)
    send_caches(WINDOWS[0])
    with jax.named_scope("permute_rest"):
        for copy in small[4:]:
            copy.wait()
        for c in (3, 0, 1):
            loads[c].wait()
            permute(c)
        for c in range(4):
            keep_own(c)
    with jax.named_scope("q_wait"):
        drain(seven(qrecv), rs_q)
    send_caches(WINDOWS[1])
    with jax.named_scope("local_attend"):
        local_attend()
    for n in range(7):
        p_copy(n).start()
    precv[me] = psend[me]
    send_caches(WINDOWS[2])
    with jax.named_scope("p_wait"):
        drain(seven(precv), rs_p)
    send_caches(WINDOWS[3])
    with jax.named_scope("merge"):
        first, second = merge(queries, fresh_k, fresh_v)

    for layer in range(2):
        if layer:
            with jax.named_scope("project"):
                block_queries(project(layer, x))
            first, second = attend(layer)
        n1 = first.shape[1]

        def out_product(which, q, size, layer=layer, first=first, second=second, n1=n1):
            at = block(which, q, size)
            return nn(first, wo[layer, :n1, at]) + nn(second, wo[layer, n1:, at])

        def between_attn(layer=layer):
            if layer:
                write_out(2)
                write_out(3)
            wait_weights(layer)

        def between_moe(layer=layer):
            if layer:
                for c, fresh in ((0, kdup), (1, vdup)):
                    a2a_wait(c)
                    for t in range(groups):
                        place_new(c, t, fresh, 0)
                    write_out(c)

        def residual_attn(q, size, layer=layer):
            if layer:
                return jnp.concatenate([fin[2 * layer - 1, core, n].astype(F32) for n in range(shot.shape[2])], axis=1)
            return hid[:, block(core, q, size)].astype(F32)

        x = all_reduce(2 * layer, out_product, residual_attn, between_attn, 1, WINDOWS[4 + 2 * layer])
        m = norm(x, gm[layer:layer + 1, :])
        with jax.named_scope("up"):
            experts_up(layer, m)

        def down_product(which, q, size, layer=layer):
            with jax.named_scope("down"):
                return nn(ubuf[...], wd[layer, :, block(which, q, size)])

        def residual_moe(q, size, layer=layer):
            return fin[2 * layer, core, q].astype(F32)

        x = all_reduce(2 * layer + 1, down_product, residual_moe, between_moe, 2, () if layer else WINDOWS[5])
    out_hid[...] = x.astype(BF16)

    with jax.named_scope("tail"):
        for r in range(4):
            drain(shot.at[r, pl.ds(0, 2)], ss_r.at[r, 0])
            drain(shot.at[r, pl.ds(0, CHIPS - 1)], ss_r.at[r, 1])
        drain(seven(qrecv), ss_q)
        drain(seven(psend), ss_p)
        for c in range(4):
            drain(sendb.at[c, pl.ds(0, len(OFFSETS))], ss_a.at[c])


def finish(*refs):
    n = len(refs) // 2
    copies = [pltpu.make_async_copy(refs[i], refs[n + i], refs[-1].at[i]) for i in range(n)]
    for copy in copies:
        copy.start()
    for copy in copies:
        copy.wait()


def solution(mesh):
    seq_spec = P('dp', 'tp', None, None)
    head_spec = P('dp', None, 'tp', None)
    col_spec = P(None, None, 'tp')
    ff_spec = P(None, None, None, 'tp')
    peers = mesh.shape['tp']

    def local_step(hidden, lengths, choice, keys_one, vals_one, keys_two, vals_two, g_attn, w_q, w_k, w_v, w_o, g_mlp, w_router, w_gate, w_up, w_down):
        rows, pos, heads, head = keys_one.shape
        dim = hidden.shape[1]
        layers, experts, ff = w_down.shape[:3]
        seq = pos * peers
        flat = lambda t: t.reshape(rows * pos * heads, head)
        turn = lambda t: jnp.swapaxes(t, -1, -2)
        wide = experts * ff
        any_spec = pl.BlockSpec(memory_space=pl.ANY)
        cache_shape = pltpu.VMEM((rows * head, seq), BF16)
        wqkv_rows = w_q.shape[2] + w_k.shape[2] + 2 * w_v.shape[2]
        scratch = [
            pltpu.SMEM((rows,), jnp.int32), pltpu.VMEM((rows, dim), BF16), pltpu.VMEM((layers, choice.shape[2], rows), jnp.int32),
            pltpu.VMEM((layers, dim), BF16), pltpu.VMEM((layers, dim), BF16),
            pltpu.VMEM((4, rows * pos * heads, head), BF16), pltpu.VMEM((4, heads, pos, rows * head), BF16),
            pltpu.VMEM((4, seq, rows * head), BF16),
            pltpu.VMEM((layers, wqkv_rows, dim), BF16), pltpu.VMEM((layers, w_o.shape[1], dim), BF16),
            pltpu.VMEM((layers, experts, dim), BF16),
            pltpu.VMEM((layers, wide, dim), BF16), pltpu.VMEM((layers, wide, dim), BF16), pltpu.VMEM((layers, wide, dim), BF16),
            pltpu.VMEM((LANES, WIDE), BF16), pltpu.VMEM((layers, rows, LANES), F32), pltpu.VMEM((layers, rows, LANES), F32),
            pltpu.VMEM((LANES, seq), F32), pltpu.VMEM((LANES, WIDE), F32),
            pltpu.VMEM((rows, wide), BF16),
            pltpu.VMEM((4, 2, rows, dim // 4), BF16), pltpu.VMEM((4, 2, rows, dim // 4), BF16),
            pltpu.VMEM((4, CHIPS, 2, rows, dim // 4), BF16), pltpu.VMEM((4, 2, 2, rows, dim // 4), BF16),
            pltpu.VMEM((heads, rows * 2, LANES), BF16), pltpu.VMEM((heads, rows * 2, LANES), F32), pltpu.VMEM((heads, rows * 2, LANES), F32),
            pltpu.SemaphoreType.DMA((7,)), pltpu.SemaphoreType.DMA((4,)), pltpu.SemaphoreType.DMA((layers, 3)),
            pltpu.SemaphoreType.DMA((layers,)),
            pltpu.SemaphoreType.DMA((4,)), pltpu.SemaphoreType.DMA((4,)),
            pltpu.SemaphoreType.DMA((4, 2)), pltpu.SemaphoreType.DMA((4, 5)),
            pltpu.SemaphoreType.DMA(()), pltpu.SemaphoreType.DMA(()), pltpu.SemaphoreType.DMA(()), pltpu.SemaphoreType.DMA(()),
        ]
        out = pl.pallas_call(
            kernel,
            name="decode_step",
            out_shape=(pltpu.VMEM((rows, dim), BF16),) + (cache_shape,) * 4,
            in_specs=[any_spec] * 17,
            out_specs=(pl.BlockSpec(memory_space=pltpu.VMEM),) * 5,
            scratch_shapes=scratch,
            compiler_params=pltpu.CompilerParams(collective_id=0, has_side_effects=True, vmem_limit_bytes=64800000),
        )(lengths, hidden, turn(choice), flat(keys_one), flat(vals_one), flat(keys_two), flat(vals_two), g_attn, turn(w_q), turn(w_k), turn(w_v), w_o,
          g_mlp, turn(w_router), turn(w_gate).reshape(layers, wide, dim), turn(w_up).reshape(layers, wide, dim), w_down.reshape(layers, wide, dim))
        out = pl.pallas_call(
            finish,
            name="finish",
            out_shape=[jax.ShapeDtypeStruct(t.shape, t.dtype) for t in out],
            in_specs=[pl.BlockSpec(memory_space=pltpu.VMEM)] * len(out),
            out_specs=[any_spec] * len(out),
            scratch_shapes=[pltpu.SemaphoreType.DMA((len(out),))],
            compiler_params=pltpu.CompilerParams(vmem_limit_bytes=1 << 20),
        )(*[pltpu.with_memory_space_constraint(t, pltpu.VMEM) for t in out])
        caches = [jnp.transpose(t.reshape(rows, head, seq), (0, 2, 1))[:, :, None, :] for t in out[1:]]
        return (out[0], *caches)

    return jax.shard_map(local_step, mesh=mesh, in_specs=(P('dp', None), P('dp'), P(None, 'dp', None), seq_spec, seq_spec, seq_spec, seq_spec, P(), col_spec, col_spec, col_spec, P(None, 'tp', None), P(), P(), ff_spec, ff_spec, P(None, None, 'tp', None)), out_specs=(P('dp', None), head_spec, head_spec, head_spec, head_spec), check_vma=False)
```

```python
import functools

import jax
import jax.numpy as jnp
from jax import lax
from jax.experimental import pallas as pl
from jax.experimental.pallas import tpu as pltpu
from jax.sharding import PartitionSpec as P

EPS = 1e-5
THETA = 1000000.0
MESH = pl.DeviceIdType.MESH
F32 = jnp.float32
BF16 = jnp.bfloat16
LANES, WIDE, TILE, HEAD = 128, 256, 16, 64
CHIPS = 4
OFFSETS = ((2, 0), (2, 1), (1, 0), (3, 0), (1, 1), (3, 1), (0, 1))
def units(cache, *which):
    pairs = ((0,), (1,), (2, 3), (4, 5), (6,))
    return [(cache, n) for k in which for n in pairs[k]]


WINDOWS = (
    units(1, 0, 1, 2, 3, 4),
    [],
    units(3, 4) + units(2, 4, 0, 1),
    units(2, 2),
    units(2, 3) + units(3, 0, 1, 2, 3),
    units(0, 4, 0, 1),
    units(0, 2, 3),
)
CHUNKS = 10


def nt(lhs, rhs):
    return lax.dot_general(lhs, rhs, (((1,), (1,)), ((), ())), preferred_element_type=F32)


def nn(lhs, rhs):
    return jnp.dot(lhs, rhs, preferred_element_type=F32)


def iota(shape, dim):
    return lax.broadcasted_iota(jnp.int32, shape, dim)


def kernel(len_h, hid_h, choice_h, k1_h, v1_h, k2_h, v2_h, ga_h, wq_h, wk_h, wv_h, wo_h, gm_h, wr_h, wg_h, wu_h, wd_h,
           out_hid, ok1, ov1, ok2, ov2,
           len_s, hid, choice, ga, gm, xst, sendb, recvb, wqkv, wo, wr, wg, wu, wd,
           qall, kdup, vdup, sc, ov, ubuf, part, d1, shot, fin, qrecv, psend, precv,
           sem_small, sem_x, sem_w, sem_wqkv, ss_a, rs_a, ss_r, rs_r, ss_q, rs_q, ss_p, rs_p):
    rows, dim = hid.shape
    half = dim // 2
    seq = recvb.shape[1]
    pos = seq // (2 * CHIPS)
    lanes = recvb.shape[2]
    groups = lanes // WIDE
    head = HEAD
    experts = wr.shape[1]
    step = wg.shape[1] // CHUNKS

    me = lax.axis_index("tp")
    chip, core = me // 2, lax.rem(me, 2)
    partner = chip * 2 + 1 - core

    def device(dx, flip):
        return lax.rem(chip + dx, CHIPS) * 2 + (1 - core if flip else core)

    def rcopy(src, dst, ssem, rsem, peer):
        return pltpu.make_async_remote_copy(src, dst, ssem, rsem, device_id={"tp": peer}, device_id_type=MESH)

    def drain(ref, sem):
        pltpu.make_async_copy(ref, ref, sem).wait()

    loads = [pltpu.make_async_copy(src, xst.at[c], sem_x.at[c]) for c, src in enumerate((k1_h, v1_h, k2_h, v2_h))]
    small = [pltpu.make_async_copy(src, dst, sem_small.at[n]) for n, (src, dst) in enumerate(
        ((hid_h, hid), (len_h, len_s), (ga_h, ga), (gm_h, gm), (choice_h, choice), (wr_h, wr), (wo_h, wo)))]

    def qkv_loads(layer):
        nq, nk = wq_h.shape[1], wk_h.shape[1]
        return [pltpu.make_async_copy(src.at[layer], wqkv.at[layer, pl.ds(at, size)], sem_wqkv.at[layer])
                for src, at, size in ((wq_h, 0, nq), (wk_h, nq, nk), (wv_h, nq + nk, nk), (wv_h, nq + 2 * nk, nk))]

    small[0].start()
    for copy in qkv_loads(0):
        copy.start()
    for copy in small[1:4]:
        copy.start()
    barrier = pltpu.get_barrier_semaphore()
    for dx, flip in OFFSETS:
        pl.semaphore_signal(barrier, inc=1, device_id={"tp": device(dx, flip)}, device_id_type=MESH)
    for c in (1, 0, 2, 3):
        loads[c].start()
    for copy in small[4:]:
        copy.start()
    for copy in qkv_loads(1):
        copy.start()

    def w_copy(layer, which, c):
        src, dst = ((wg_h, wg), (wu_h, wu), (wd_h, wd))[which]
        at = pl.ds(pl.multiple_of(c * step, step), step)
        return pltpu.make_async_copy(src.at[layer, at], dst.at[layer, at], sem_w.at[layer, which])

    def permute(c):
        i, j = iota((LANES, LANES), 0), iota((LANES, LANES), 1)
        perm = (j == lax.rem(i, TILE) * 8 + i // TILE).astype(BF16)

        for t in range(groups):
            tiles = [xst[c, slice(t * 512 + n * LANES, t * 512 + n * LANES + LANES), :] for n in range(4)]
            moved = nn(perm, jnp.concatenate(tiles, axis=1)).astype(BF16)
            sendb[c, :, :, slice(t * WIDE, t * WIDE + WIDE)] = moved.reshape(8, pos, WIDE)

    def a2a_copy(c, n):
        peer = device(*OFFSETS[n])
        return rcopy(sendb.at[c, peer], recvb.at[c, pl.ds(pl.multiple_of(me * pos, pos), pos)], ss_a.at[c], rs_a.at[c], peer)

    def a2a_wait(c):
        drain(recvb.at[c, pl.ds(0, len(OFFSETS) * pos)], rs_a.at[c])

    def keep_own(c):
        recvb[c, pl.ds(pl.multiple_of(me * pos, pos), pos), :] = sendb[c, me]

    for layer in range(2):
        def start_weights(c, _, layer=layer):
            w_copy(layer, 0, c).start()
            w_copy(layer, 1, c).start()
            w_copy(layer, 2, c).start()
            return 0
        lax.fori_loop(0, CHUNKS, start_weights, 0)

    with jax.named_scope("small_wait"):
        for copy in small[:4]:
            copy.wait()
    lane = iota((rows, LANES), 1)
    row = iota((rows, LANES), 0)
    len_f = jnp.zeros((rows, LANES), F32)
    for b in range(rows):
        len_f = jnp.where(row == b, len_s[b].astype(F32), len_f)
    freq = jnp.exp(lax.rem(lane, 32).astype(F32) * (-2.0 / head * 13.815510557964274))
    angle = len_f * freq
    cos_t, sin_t = jnp.cos(angle), jnp.sin(angle)
    low = lax.rem(lane, head) < head // 2
    left = lane < head

    def rope(x):
        turned = jnp.where(low, -pltpu.roll(x, 96, 1), pltpu.roll(x, 32, 1))
        return (x * cos_t + turned * sin_t).astype(BF16).astype(F32)

    def norm(x, gain):
        scale = lax.rsqrt(jnp.mean(x * x, axis=-1, keepdims=True) + EPS)
        return (x * scale * gain.astype(F32)).astype(BF16)

    def project(layer, x):
        drain(wqkv.at[layer], sem_wqkv.at[layer])
        qkv = nt(norm(x, ga[layer:layer + 1, :]), wqkv[layer])
        t0, t1 = rope(qkv[:, :LANES]), rope(qkv[:, LANES:WIDE])
        s0, s1 = pltpu.roll(t0, HEAD, 1), pltpu.roll(t1, HEAD, 1)
        q3 = jnp.concatenate([jnp.where(left, t0, s0), jnp.where(left, s0, t0), jnp.where(left, t1, s1)], axis=0).astype(BF16)
        kdup[layer] = jnp.where(left, s1, t1)
        vdup[layer] = qkv[:, WIDE:384].astype(BF16).astype(F32)
        return q3

    def block_queries(q3):
        i, j = iota((LANES, 96), 0), iota((LANES, 96), 1)
        slot = lax.rem(i, TILE)
        pick = (lax.rem(slot, 4) < 3) & (j == lax.rem(slot, 4) * rows + i // 4)
        dup = nn(pick.astype(BF16), q3)
        slot2, lane2 = lax.rem(iota((LANES, WIDE), 0), TILE), iota((LANES, WIDE), 1)
        both = jnp.concatenate([dup, dup], axis=1)
        qall[...] = jnp.where(slot2 // 4 == lane2 // HEAD, both, 0.0).astype(BF16)

    hb = rows // 2
    prow, plane = iota((hb * 4, LANES), 0), iota((hb * 4, LANES), 1)
    pleft = plane < head

    def pack(table, cells):
        width = table.shape[0]
        i, j = iota((hb * 4, width), 0), iota((hb * 4, width), 1)
        low_half = nn(cells(i, j, 0).astype(BF16), table)
        high_half = nn(cells(i, j, hb).astype(BF16), table)
        return jnp.where(pleft, low_half, high_half)

    def pack_queries(q3):
        return pack(q3, lambda i, j, b0: (lax.rem(i, 4) < 3) & (j == lax.rem(i, 4) * rows + i // 4 + b0))

    def pack_fresh(table):
        return pack(table.astype(BF16), lambda i, j, b0: j == i // 4 + b0)

    def to_all(n, src, dst, ssem, rsem):
        return rcopy(src, dst, ssem, rsem, device(*OFFSETS[n]))

    def q_copy(n):
        return to_all(n, qrecv.at[me], qrecv.at[me], ss_q, rs_q)

    def p_copy(n):
        return to_all(n, psend.at[device(*OFFSETS[n])], precv.at[me], ss_p, rs_p)

    def seven(ref):
        return ref.at[pl.ds(0, len(OFFSETS))]

    def local_scores():
        wide_row, wide_lane = iota((LANES, WIDE), 0), iota((LANES, WIDE), 1)
        diagonal = wide_lane // head == lax.rem(wide_row, TILE) // 4
        half_lane = iota((LANES, LANES), 1) < head
        lane_block = iota((TILE, LANES), 1) // pos
        kept = [jnp.zeros((TILE, LANES), F32)] * 8
        for t in range(groups):
            at = slice(t % 4 * TILE, t % 4 * TILE + TILE)
            q = qrecv[:, at, :].reshape(LANES, LANES).astype(F32)
            q = jnp.where(half_lane if t < 4 else ~half_lane, q, 0.0)
            q = q + pltpu.roll(q, HEAD, 1)
            q = jnp.where(diagonal, jnp.concatenate([q, q], axis=1), 0.0).astype(BF16)
            keys = sendb[0, :, :, t * WIDE:(t + 1) * WIDE].reshape(LANES, WIDE)
            s = nt(q, keys) * (head ** -0.5)
            for h in range(8):
                turned = s[h * TILE:(h + 1) * TILE, :]
                if h != t:
                    turned = pltpu.roll(turned, (t - h) % 8 * pos, 1)
                kept[h] = jnp.where(lane_block == t, turned, kept[h])
        for h in range(8):
            psend[h] = kept[h]

    def half_sum(x):
        low_half = jnp.sum(jnp.where(pleft, x, 0.0), axis=-1, keepdims=True)
        high_half = jnp.sum(jnp.where(pleft, 0.0, x), axis=-1, keepdims=True)
        return jnp.where(pleft, low_half, high_half)

    def gathered_scores(own):
        lane_block = iota((TILE, LANES), 1) // pos
        for t in range(groups):
            tile = precv[t]
            for j in range(2 * CHIPS):
                turned = precv[j]
                if j != t:
                    turned = pltpu.roll(turned, (j - t) % 8 * pos, 1)
                tile = jnp.where(lane_block == j, turned, tile)
            sc[t * TILE:(t + 1) * TILE, :] = tile
        fresh = jnp.concatenate([own[:, :1], own[:, head:head + 1]], axis=0)
        limit = jnp.zeros((LANES, LANES), jnp.int32)
        row_i, lane_i = iota((LANES, LANES), 0) // 4, iota((LANES, LANES), 1)
        for b in range(rows):
            limit = jnp.where(row_i == b, len_s[b], limit)
        s = jnp.where(lane_i == limit, fresh, sc[...])
        return jnp.where(lane_i <= limit, s, -1e30)

    def place_new(c, t, fresh, layer):
        at = slice(t * WIDE, t * WIDE + WIDE)
        pos_i, lane_i = iota((seq, LANES), 0), iota((seq, LANES), 1)
        pieces = []
        for n in range(2):
            first = t * 4 + 2 * n
            where_new = jnp.where(lane_i < head, len_s[first], len_s[first + 1])
            line = jnp.where(lane_i[:1] < head, fresh[layer, first:first + 1, :], fresh[layer, first + 1:first + 2, :])
            old = recvb[c, :, slice(t * WIDE + n * LANES, t * WIDE + n * LANES + LANES)].astype(F32)
            pieces.append(jnp.where(pos_i == where_new, line, old))
        tile = jnp.concatenate(pieces, axis=1).astype(BF16)
        recvb[c, :, at] = tile
        return tile

    def layer_scores(layer):
        ck = 2 * layer
        with jax.named_scope("wait_keys"):
            a2a_wait(ck)

        def scores(t):
            tile = place_new(ck, t, kdup, layer)
            at = slice(t * TILE, t * TILE + TILE)
            s = nt(qall[at, :], tile) * (head ** -0.5)
            slot, p = iota((TILE, seq), 0) // 4, iota((TILE, seq), 1)
            limit = jnp.where(slot == 0, len_s[4 * t], jnp.where(slot == 1, len_s[4 * t + 1], jnp.where(slot == 2, len_s[4 * t + 2], len_s[4 * t + 3])))
            sc[at, :] = jnp.where(p <= limit, s, -1e30)
        with jax.named_scope("scores"):
            for t in range(groups):
                scores(t)
        return sc[...]

    def attend(layer, s):
        cv = 2 * layer + 1
        e = jnp.exp(s - jnp.max(s, axis=-1, keepdims=True))
        sc[...] = e / jnp.sum(e, axis=-1, keepdims=True)
        with jax.named_scope("wait_values"):
            a2a_wait(cv)

        def values(t):
            tile = place_new(cv, t, vdup, layer)
            at = slice(t * TILE, t * TILE + TILE)
            ov[at, :] = nn(sc[at, :].astype(BF16), tile)
        with jax.named_scope("values"):
            for t in range(groups):
                values(t)
        slot2, lane2 = lax.rem(iota((LANES, WIDE), 0), TILE), iota((LANES, WIDE), 1)
        kept = jnp.where(slot2 // 4 == lane2 // HEAD, ov[...], 0.0)
        both = (kept[:, :LANES] + kept[:, LANES:]).astype(BF16)
        i, j = iota((rows, LANES), 0), iota((rows, LANES), 1)
        per_head = []
        for r in range(3):
            got = nn((j == i * 4 + r).astype(BF16), both)
            per_head.append(got + pltpu.roll(got, HEAD, 1))
        return jnp.where(left, per_head[0], per_head[1]).astype(BF16), per_head[2].astype(BF16)[:, :head]

    outs = (ok1, ov1, ok2, ov2)

    def write_out(c):
        for t in range(groups):
            outs[c][t * WIDE:(t + 1) * WIDE, :] = recvb[c, :, t * WIDE:(t + 1) * WIDE].T

    def cols(which):
        return pl.ds(pl.multiple_of(which * half, half), half)

    def block(which, q, size):
        return pl.ds(pl.multiple_of(which * half + q * size, size), size)

    def all_reduce(r, product, residual, between, parts, window):
        size = half // parts
        per = shot.shape[2] // parts

        def send(ref, dst, ssem, rsem, peer):
            rcopy(ref, dst, ss_r.at[r, ssem], rs_r.at[r, rsem], peer).start()

        def put(ref, q, value):
            for n in range(per):
                ref[q * per + n] = value[:, n * (size // per):(n + 1) * (size // per)].astype(BF16)

        def get(ref, q):
            return jnp.concatenate([ref[q * per + n].astype(F32) for n in range(per)], axis=1)

        for q in range(parts):
            put(part.at[r], q, product(1 - core, q, size))
            at = pl.ds(q * per, per)
            send(part.at[r, at], d1.at[r, at], 0, q, partner)
        for q in range(parts):
            mine = product(core, q, size)
            with jax.named_scope("swap_wait"):
                drain(d1.at[r, pl.ds(q * per, per)], rs_r.at[r, q])
            put(shot.at[r, chip], q, mine + get(d1.at[r], q))
            piece = shot.at[r, chip, pl.ds(q * per, per)]
            for dx in (2, 1, 3):
                send(piece, piece, 1, 2 + q, device(dx, 0))
        with jax.named_scope("between"):
            between()
        for q in range(parts):
            at = pl.ds(q * per, per)
            with jax.named_scope("shot_wait"):
                drain(shot.at[r, pl.ds(0, CHIPS - 1), at], rs_r.at[r, 2 + q])
            total = (get(shot.at[r, 0], q) + get(shot.at[r, 1], q)) + (get(shot.at[r, 2], q) + get(shot.at[r, 3], q))
            put(fin.at[r, core], q, residual(q, size) + total)
            send(fin.at[r, core, at], fin.at[r, core, at], 0, 4, partner)
        send_caches(window)
        with jax.named_scope("last_wait"):
            drain(fin.at[r, 1 - core], rs_r.at[r, 4])
        pieces = [fin[r, h, n].astype(F32) for h in range(2) for n in range(shot.shape[2])]
        return jnp.concatenate(pieces, axis=1)

    def gates(layer, m):
        logits = nt(wr[layer], m)
        e_i = iota((experts, rows), 0)
        chosen = e_i == choice[layer, 0:1, :]
        for n in range(1, choice.shape[1]):
            chosen = chosen | (e_i == choice[layer, n:n + 1, :])
        top = jnp.max(jnp.where(chosen, logits, -3e38), axis=0, keepdims=True)
        weight = jnp.where(chosen, jnp.exp(jnp.where(chosen, logits - top, 0.0)), 0.0)
        return (weight / jnp.sum(weight, axis=0, keepdims=True)).T

    def wait_weights(layer):
        for which, ref in enumerate((wg, wu, wd)):
            drain(ref.at[layer], sem_w.at[layer, which])

    def experts_up(layer, m):
        gate = gates(layer, m)
        pairs = step // LANES
        for c in range(CHUNKS):
            at = slice(c * step, (c + 1) * step)
            g = nt(m, wg[layer, at, :])
            up = nt(wu[layer, at, :], m).T
            wide = jnp.concatenate([jnp.where(left, gate[:, 2 * n:2 * n + 1], gate[:, 2 * n + 1:2 * n + 2]) for n in range(c * pairs, (c + 1) * pairs)], axis=1)
            ubuf[:, at] = (jax.nn.silu(g) * up * wide).astype(BF16)

    def send_caches(wanted):
        for c, n in wanted:
            a2a_copy(c, n).start()

    x = hid[...].astype(F32)
    with jax.named_scope("project"):
        q3 = project(0, x)
        queries = pack_queries(q3)
        qrecv[me] = queries.astype(BF16)
    with jax.named_scope("barrier"):
        pl.semaphore_wait(barrier, len(OFFSETS))
    for n in range(7):
        q_copy(n).start()
    with jax.named_scope("permute1"):
        loads[1].wait()
        permute(1)
    with jax.named_scope("permute_rest"):
        loads[0].wait()
        permute(0)
    send_caches(WINDOWS[0])
    with jax.named_scope("own_score"):
        own_score = half_sum(queries * pack_fresh(kdup[0])) * (head ** -0.5)
    with jax.named_scope("permute23"):
        for copy in small[4:]:
            copy.wait()
        for c in (2, 3):
            loads[c].wait()
            permute(c)
        for c in range(4):
            keep_own(c)
    with jax.named_scope("q_wait"):
        drain(seven(qrecv), rs_q)
    send_caches(WINDOWS[1])
    with jax.named_scope("local_scores"):
        local_scores()
    for n in range(7):
        p_copy(n).start()
    send_caches(WINDOWS[2])
    precv[me] = psend[me]
    with jax.named_scope("p_wait"):
        drain(seven(precv), rs_p)
    send_caches(WINDOWS[3])
    with jax.named_scope("merge"):
        s = gathered_scores(own_score)

    for layer in range(2):
        if layer:
            with jax.named_scope("project"):
                block_queries(project(layer, x))
            s = layer_scores(layer)
        first, second = attend(layer, s)
        n1 = first.shape[1]

        def out_product(which, q, size, layer=layer, first=first, second=second, n1=n1):
            at = block(which, q, size)
            return nn(first, wo[layer, :n1, at]) + nn(second, wo[layer, n1:, at])

        def between_attn(layer=layer):
            if layer:
                write_out(2)
                write_out(3)
            else:
                write_out(1)
            wait_weights(layer)

        def between_moe(layer=layer):
            if layer:
                a2a_wait(0)
                for t in range(groups):
                    place_new(0, t, kdup, 0)
                write_out(0)

        def residual_attn(q, size, layer=layer):
            if layer:
                return jnp.concatenate([fin[2 * layer - 1, core, n].astype(F32) for n in range(shot.shape[2])], axis=1)
            return hid[:, block(core, q, size)].astype(F32)

        x = all_reduce(2 * layer, out_product, residual_attn, between_attn, 1, WINDOWS[4 + 2 * layer])
        m = norm(x, gm[layer:layer + 1, :])
        with jax.named_scope("up"):
            experts_up(layer, m)

        def down_product(which, q, size, layer=layer):
            with jax.named_scope("down"):
                return nn(ubuf[...], wd[layer, :, block(which, q, size)])

        def residual_moe(q, size, layer=layer):
            return fin[2 * layer, core, q].astype(F32)

        x = all_reduce(2 * layer + 1, down_product, residual_moe, between_moe, 2, () if layer else WINDOWS[5])
    out_hid[...] = x.astype(BF16)

    with jax.named_scope("tail"):
        for r in range(4):
            drain(shot.at[r, pl.ds(0, 2)], ss_r.at[r, 0])
            drain(shot.at[r, pl.ds(0, CHIPS - 1)], ss_r.at[r, 1])
        drain(seven(qrecv), ss_q)
        drain(seven(psend), ss_p)
        for c in range(4):
            drain(sendb.at[c, pl.ds(0, len(OFFSETS))], ss_a.at[c])


def finish(*refs):
    n = len(refs) // 2
    copies = [pltpu.make_async_copy(refs[i], refs[n + i], refs[-1].at[i]) for i in range(n)]
    for copy in copies:
        copy.start()
    for copy in copies:
        copy.wait()


def solution(mesh):
    seq_spec = P('dp', 'tp', None, None)
    head_spec = P('dp', None, 'tp', None)
    col_spec = P(None, None, 'tp')
    ff_spec = P(None, None, None, 'tp')
    peers = mesh.shape['tp']

    def local_step(hidden, lengths, choice, keys_one, vals_one, keys_two, vals_two, g_attn, w_q, w_k, w_v, w_o, g_mlp, w_router, w_gate, w_up, w_down):
        rows, pos, heads, head = keys_one.shape
        dim = hidden.shape[1]
        layers, experts, ff = w_down.shape[:3]
        seq = pos * peers
        flat = lambda t: t.reshape(rows * pos * heads, head)
        turn = lambda t: jnp.swapaxes(t, -1, -2)
        wide = experts * ff
        any_spec = pl.BlockSpec(memory_space=pl.ANY)
        cache_shape = pltpu.VMEM((rows * head, seq), BF16)
        wqkv_rows = w_q.shape[2] + w_k.shape[2] + 2 * w_v.shape[2]
        scratch = [
            pltpu.SMEM((rows,), jnp.int32), pltpu.VMEM((rows, dim), BF16), pltpu.VMEM((layers, choice.shape[2], rows), jnp.int32),
            pltpu.VMEM((layers, dim), BF16), pltpu.VMEM((layers, dim), BF16),
            pltpu.VMEM((4, rows * pos * heads, head), BF16), pltpu.VMEM((4, heads, pos, rows * head), BF16),
            pltpu.VMEM((4, seq, rows * head), BF16),
            pltpu.VMEM((layers, wqkv_rows, dim), BF16), pltpu.VMEM((layers, w_o.shape[1], dim), BF16),
            pltpu.VMEM((layers, experts, dim), BF16),
            pltpu.VMEM((layers, wide, dim), BF16), pltpu.VMEM((layers, wide, dim), BF16), pltpu.VMEM((layers, wide, dim), BF16),
            pltpu.VMEM((LANES, WIDE), BF16), pltpu.VMEM((layers, rows, LANES), F32), pltpu.VMEM((layers, rows, LANES), F32),
            pltpu.VMEM((LANES, seq), F32), pltpu.VMEM((LANES, WIDE), F32),
            pltpu.VMEM((rows, wide), BF16),
            pltpu.VMEM((4, 2, rows, dim // 4), BF16), pltpu.VMEM((4, 2, rows, dim // 4), BF16),
            pltpu.VMEM((4, CHIPS, 2, rows, dim // 4), BF16), pltpu.VMEM((4, 2, 2, rows, dim // 4), BF16),
            pltpu.VMEM((heads, rows * 2, LANES), BF16), pltpu.VMEM((heads, TILE, LANES), F32), pltpu.VMEM((heads, TILE, LANES), F32),
            pltpu.SemaphoreType.DMA((7,)), pltpu.SemaphoreType.DMA((4,)), pltpu.SemaphoreType.DMA((layers, 3)),
            pltpu.SemaphoreType.DMA((layers,)),
            pltpu.SemaphoreType.DMA((4,)), pltpu.SemaphoreType.DMA((4,)),
            pltpu.SemaphoreType.DMA((4, 2)), pltpu.SemaphoreType.DMA((4, 5)),
            pltpu.SemaphoreType.DMA(()), pltpu.SemaphoreType.DMA(()), pltpu.SemaphoreType.DMA(()), pltpu.SemaphoreType.DMA(()),
        ]
        out = pl.pallas_call(
            kernel,
            name="decode_step",
            out_shape=(pltpu.VMEM((rows, dim), BF16),) + (cache_shape,) * 4,
            in_specs=[any_spec] * 17,
            out_specs=(pl.BlockSpec(memory_space=pltpu.VMEM),) * 5,
            scratch_shapes=scratch,
            compiler_params=pltpu.CompilerParams(collective_id=0, has_side_effects=True, vmem_limit_bytes=64800000),
        )(lengths, hidden, turn(choice), flat(keys_one), flat(vals_one), flat(keys_two), flat(vals_two), g_attn, turn(w_q), turn(w_k), turn(w_v), w_o,
          g_mlp, turn(w_router), turn(w_gate).reshape(layers, wide, dim), turn(w_up).reshape(layers, wide, dim), w_down.reshape(layers, wide, dim))
        out = pl.pallas_call(
            finish,
            name="finish",
            out_shape=[jax.ShapeDtypeStruct(t.shape, t.dtype) for t in out],
            in_specs=[pl.BlockSpec(memory_space=pltpu.VMEM)] * len(out),
            out_specs=[any_spec] * len(out),
            scratch_shapes=[pltpu.SemaphoreType.DMA((len(out),))],
            compiler_params=pltpu.CompilerParams(vmem_limit_bytes=1 << 20),
        )(*[pltpu.with_memory_space_constraint(t, pltpu.VMEM) for t in out])
        caches = [jnp.transpose(t.reshape(rows, head, seq), (0, 2, 1))[:, :, None, :] for t in out[1:]]
        return (out[0], *caches)

    return jax.shard_map(local_step, mesh=mesh, in_specs=(P('dp', None), P('dp'), P(None, 'dp', None), seq_spec, seq_spec, seq_spec, seq_spec, P(), col_spec, col_spec, col_spec, P(None, 'tp', None), P(), P(), ff_spec, ff_spec, P(None, None, 'tp', None)), out_specs=(P('dp', None), head_spec, head_spec, head_spec, head_spec), check_vma=False)
```

```python
import functools

import jax
import jax.numpy as jnp
from jax import lax
from jax.experimental import pallas as pl
from jax.experimental.pallas import tpu as pltpu
from jax.sharding import PartitionSpec as P

EPS = 1e-5
THETA = 1000000.0
MESH = pl.DeviceIdType.MESH
F32 = jnp.float32
BF16 = jnp.bfloat16
LANES, WIDE, TILE, HEAD = 128, 256, 16, 64
CHIPS = 4
OFFSETS = ((2, 0), (2, 1), (1, 0), (3, 0), (1, 1), (3, 1), (0, 1))
def units(cache, *which):
    pairs = ((0,), (1,), (2, 3), (4, 5), (6,))
    return [(cache, n) for k in which for n in pairs[k]]


WINDOWS = (
    units(1, 2, 3, 0, 1, 4),
    [],
    units(3, 4) + units(2, 4, 0, 1),
    units(2, 2),
    units(2, 3) + units(3, 0, 1, 2, 3),
    units(0, 4, 0, 1),
    units(0, 2, 3),
)
CHUNKS = 10


def nt(lhs, rhs):
    return lax.dot_general(lhs, rhs, (((1,), (1,)), ((), ())), preferred_element_type=F32)


def nn(lhs, rhs):
    return jnp.dot(lhs, rhs, preferred_element_type=F32)


def iota(shape, dim):
    return lax.broadcasted_iota(jnp.int32, shape, dim)


def kernel(len_h, hid_h, choice_h, k1_h, v1_h, k2_h, v2_h, ga_h, wq_h, wk_h, wv_h, wo_h, gm_h, wr_h, wg_h, wu_h, wd_h,
           out_hid, ok1, ov1, ok2, ov2,
           len_s, hid, choice, ga, gm, xst, sendb, recvb, wqkv, wo, wr, wg, wu, wd,
           qall, kdup, vdup, turns, sc, ov, ubuf, part, d1, shot, fin, qrecv, psend, precv,
           sem_small, sem_x, sem_w, sem_wqkv, ss_a, rs_a, ss_r, rs_r, ss_q, rs_q, ss_p, rs_p):
    rows, dim = hid.shape
    half = dim // 2
    seq = recvb.shape[1]
    pos = seq // (2 * CHIPS)
    lanes = recvb.shape[2]
    groups = lanes // WIDE
    head = HEAD
    experts = wr.shape[1]
    step = wg.shape[1] // CHUNKS

    me = lax.axis_index("tp")
    chip, core = me // 2, lax.rem(me, 2)
    partner = chip * 2 + 1 - core

    def device(dx, flip):
        return lax.rem(chip + dx, CHIPS) * 2 + (1 - core if flip else core)

    def rcopy(src, dst, ssem, rsem, peer):
        return pltpu.make_async_remote_copy(src, dst, ssem, rsem, device_id={"tp": peer}, device_id_type=MESH)

    def drain(ref, sem):
        pltpu.make_async_copy(ref, ref, sem).wait()

    loads = [pltpu.make_async_copy(src, xst.at[c], sem_x.at[c]) for c, src in enumerate((k1_h, v1_h, k2_h, v2_h))]
    small = [pltpu.make_async_copy(src, dst, sem_small.at[n]) for n, (src, dst) in enumerate(
        ((len_h, len_s), (hid_h, hid), (ga_h, ga), (gm_h, gm), (choice_h, choice), (wr_h, wr), (wo_h, wo)))]

    def qkv_loads(layer):
        nq, nk = wq_h.shape[1], wk_h.shape[1]
        return [pltpu.make_async_copy(src.at[layer], wqkv.at[layer, pl.ds(at, size)], sem_wqkv.at[layer])
                for src, at, size in ((wq_h, 0, nq), (wk_h, nq, nk), (wv_h, nq + nk, nk), (wv_h, nq + 2 * nk, nk))]

    for copy in small[:2]:
        copy.start()
    for copy in qkv_loads(0):
        copy.start()
    for copy in small[2:4]:
        copy.start()
    barrier = pltpu.get_barrier_semaphore()
    for dx, flip in OFFSETS:
        pl.semaphore_signal(barrier, inc=1, device_id={"tp": device(dx, flip)}, device_id_type=MESH)
    for c in (1, 0, 2, 3):
        loads[c].start()
    for copy in small[4:]:
        copy.start()
    for copy in qkv_loads(1):
        copy.start()

    def w_copy(layer, which, c):
        src, dst = ((wg_h, wg), (wu_h, wu), (wd_h, wd))[which]
        at = pl.ds(pl.multiple_of(c * step, step), step)
        return pltpu.make_async_copy(src.at[layer, at], dst.at[layer, at], sem_w.at[layer, which])

    def permute(c):
        i, j = iota((LANES, LANES), 0), iota((LANES, LANES), 1)
        perm = (j == lax.rem(i, TILE) * 8 + i // TILE).astype(BF16)

        for t in range(groups):
            tiles = [xst[c, slice(t * 512 + n * LANES, t * 512 + n * LANES + LANES), :] for n in range(4)]
            moved = nn(perm, jnp.concatenate(tiles, axis=1)).astype(BF16)
            sendb[c, :, :, slice(t * WIDE, t * WIDE + WIDE)] = moved.reshape(8, pos, WIDE)

    def a2a_copy(c, n):
        peer = device(*OFFSETS[n])
        return rcopy(sendb.at[c, peer], recvb.at[c, pl.ds(pl.multiple_of(me * pos, pos), pos)], ss_a.at[c], rs_a.at[c], peer)

    def a2a_wait(c):
        drain(recvb.at[c, pl.ds(0, len(OFFSETS) * pos)], rs_a.at[c])

    def keep_own(c):
        recvb[c, pl.ds(pl.multiple_of(me * pos, pos), pos), :] = sendb[c, me]

    for layer in range(2):
        def start_weights(c, _, layer=layer):
            w_copy(layer, 0, c).start()
            w_copy(layer, 1, c).start()
            w_copy(layer, 2, c).start()
            return 0
        lax.fori_loop(0, CHUNKS, start_weights, 0)

    with jax.named_scope("len_wait"):
        small[0].wait()
    lane = iota((rows, LANES), 1)
    row = iota((rows, LANES), 0)
    len_f = jnp.zeros((rows, LANES), F32)
    for b in range(rows):
        len_f = jnp.where(row == b, len_s[b].astype(F32), len_f)
    freq = jnp.exp(lax.rem(lane, 32).astype(F32) * (-2.0 / head * 13.815510557964274))
    angle = len_f * freq
    turns[0], turns[1] = jnp.cos(angle), jnp.sin(angle)
    low = lax.rem(lane, head) < head // 2
    left = lane < head

    def rope(x):
        turned = jnp.where(low, -pltpu.roll(x, 96, 1), pltpu.roll(x, 32, 1))
        return (x * turns[0] + turned * turns[1]).astype(BF16).astype(F32)

    def norm(x, gain):
        scale = lax.rsqrt(jnp.mean(x * x, axis=-1, keepdims=True) + EPS)
        return (x * scale * gain.astype(F32)).astype(BF16)

    def project(layer, x):
        drain(wqkv.at[layer], sem_wqkv.at[layer])
        qkv = nt(norm(x, ga[layer:layer + 1, :]), wqkv[layer])
        t0, t1 = rope(qkv[:, :LANES]), rope(qkv[:, LANES:WIDE])
        s0, s1 = pltpu.roll(t0, HEAD, 1), pltpu.roll(t1, HEAD, 1)
        q3 = jnp.concatenate([jnp.where(left, t0, s0), jnp.where(left, s0, t0), jnp.where(left, t1, s1)], axis=0).astype(BF16)
        kdup[layer] = jnp.where(left, s1, t1)
        vdup[layer] = qkv[:, WIDE:384].astype(BF16).astype(F32)
        return q3

    def block_queries(q3):
        i, j = iota((LANES, 96), 0), iota((LANES, 96), 1)
        slot = lax.rem(i, TILE)
        pick = (lax.rem(slot, 4) < 3) & (j == lax.rem(slot, 4) * rows + i // 4)
        dup = nn(pick.astype(BF16), q3)
        slot2, lane2 = lax.rem(iota((LANES, WIDE), 0), TILE), iota((LANES, WIDE), 1)
        both = jnp.concatenate([dup, dup], axis=1)
        qall[...] = jnp.where(slot2 // 4 == lane2 // HEAD, both, 0.0).astype(BF16)

    hb = rows // 2
    prow, plane = iota((hb * 4, LANES), 0), iota((hb * 4, LANES), 1)
    pleft = plane < head

    def pack(table, cells):
        width = table.shape[0]
        i, j = iota((hb * 4, width), 0), iota((hb * 4, width), 1)
        low_half = nn(cells(i, j, 0).astype(BF16), table)
        high_half = nn(cells(i, j, hb).astype(BF16), table)
        return jnp.where(pleft, low_half, high_half)

    def pack_queries(q3):
        return pack(q3, lambda i, j, b0: (lax.rem(i, 4) < 3) & (j == lax.rem(i, 4) * rows + i // 4 + b0))

    def pack_fresh(table):
        return pack(table.astype(BF16), lambda i, j, b0: j == i // 4 + b0)

    def to_all(n, src, dst, ssem, rsem):
        return rcopy(src, dst, ssem, rsem, device(*OFFSETS[n]))

    def q_copy(n):
        return to_all(n, qrecv.at[me], qrecv.at[me], ss_q, rs_q)

    def p_copy(n):
        return to_all(n, psend.at[device(*OFFSETS[n])], precv.at[me], ss_p, rs_p)

    def seven(ref):
        return ref.at[pl.ds(0, len(OFFSETS))]

    def local_scores():
        wide_row, wide_lane = iota((LANES, WIDE), 0), iota((LANES, WIDE), 1)
        diagonal = wide_lane // head == lax.rem(wide_row, TILE) // 4
        half_lane = iota((LANES, LANES), 1) < head
        lane_block = iota((TILE, LANES), 1) // pos
        kept = [jnp.zeros((TILE, LANES), F32)] * 8
        for t in range(groups):
            at = slice(t % 4 * TILE, t % 4 * TILE + TILE)
            q = qrecv[:, at, :].reshape(LANES, LANES).astype(F32)
            q = jnp.where(half_lane if t < 4 else ~half_lane, q, 0.0)
            q = q + pltpu.roll(q, HEAD, 1)
            q = jnp.where(diagonal, jnp.concatenate([q, q], axis=1), 0.0).astype(BF16)
            keys = sendb[0, :, :, t * WIDE:(t + 1) * WIDE].reshape(LANES, WIDE)
            s = nt(q, keys) * (head ** -0.5)
            for h in range(8):
                turned = s[h * TILE:(h + 1) * TILE, :]
                if h != t:
                    turned = pltpu.roll(turned, (t - h) % 8 * pos, 1)
                kept[h] = jnp.where(lane_block == t, turned, kept[h])
        for h in range(8):
            psend[h] = kept[h]

    def half_sum(x):
        low_half = jnp.sum(jnp.where(pleft, x, 0.0), axis=-1, keepdims=True)
        high_half = jnp.sum(jnp.where(pleft, 0.0, x), axis=-1, keepdims=True)
        return jnp.where(pleft, low_half, high_half)

    def gathered_scores(own):
        lane_block = iota((TILE, LANES), 1) // pos
        for t in range(groups):
            tile = precv[t]
            for j in range(2 * CHIPS):
                turned = precv[j]
                if j != t:
                    turned = pltpu.roll(turned, (j - t) % 8 * pos, 1)
                tile = jnp.where(lane_block == j, turned, tile)
            sc[t * TILE:(t + 1) * TILE, :] = tile
        fresh = jnp.concatenate([own[:, :1], own[:, head:head + 1]], axis=0)
        limit = jnp.zeros((LANES, LANES), jnp.int32)
        row_i, lane_i = iota((LANES, LANES), 0) // 4, iota((LANES, LANES), 1)
        for b in range(rows):
            limit = jnp.where(row_i == b, len_s[b], limit)
        s = jnp.where(lane_i == limit, fresh, sc[...])
        return jnp.where(lane_i <= limit, s, -1e30)

    def place_new(c, t, fresh, layer):
        at = slice(t * WIDE, t * WIDE + WIDE)
        pos_i, lane_i = iota((seq, LANES), 0), iota((seq, LANES), 1)
        pieces = []
        for n in range(2):
            first = t * 4 + 2 * n
            where_new = jnp.where(lane_i < head, len_s[first], len_s[first + 1])
            line = jnp.where(lane_i[:1] < head, fresh[layer, first:first + 1, :], fresh[layer, first + 1:first + 2, :])
            old = recvb[c, :, slice(t * WIDE + n * LANES, t * WIDE + n * LANES + LANES)].astype(F32)
            pieces.append(jnp.where(pos_i == where_new, line, old))
        tile = jnp.concatenate(pieces, axis=1).astype(BF16)
        recvb[c, :, at] = tile
        return tile

    def layer_scores(layer):
        ck = 2 * layer
        with jax.named_scope("wait_keys"):
            a2a_wait(ck)

        def scores(t):
            tile = place_new(ck, t, kdup, layer)
            at = slice(t * TILE, t * TILE + TILE)
            s = nt(qall[at, :], tile) * (head ** -0.5)
            slot, p = iota((TILE, seq), 0) // 4, iota((TILE, seq), 1)
            limit = jnp.where(slot == 0, len_s[4 * t], jnp.where(slot == 1, len_s[4 * t + 1], jnp.where(slot == 2, len_s[4 * t + 2], len_s[4 * t + 3])))
            sc[at, :] = jnp.where(p <= limit, s, -1e30)
        with jax.named_scope("scores"):
            for t in range(groups):
                scores(t)
        return sc[...]

    def attend(layer, s):
        cv = 2 * layer + 1
        e = jnp.exp(s - jnp.max(s, axis=-1, keepdims=True))
        sc[...] = e / jnp.sum(e, axis=-1, keepdims=True)
        with jax.named_scope("wait_values"):
            a2a_wait(cv)

        def values(t):
            tile = place_new(cv, t, vdup, layer)
            at = slice(t * TILE, t * TILE + TILE)
            ov[at, :] = nn(sc[at, :].astype(BF16), tile)
        with jax.named_scope("values"):
            for t in range(groups):
                values(t)
        slot2, lane2 = lax.rem(iota((LANES, WIDE), 0), TILE), iota((LANES, WIDE), 1)
        kept = jnp.where(slot2 // 4 == lane2 // HEAD, ov[...], 0.0)
        both = (kept[:, :LANES] + kept[:, LANES:]).astype(BF16)
        i, j = iota((rows, LANES), 0), iota((rows, LANES), 1)
        per_head = []
        for r in range(3):
            got = nn((j == i * 4 + r).astype(BF16), both)
            per_head.append(got + pltpu.roll(got, HEAD, 1))
        return jnp.where(left, per_head[0], per_head[1]).astype(BF16), per_head[2].astype(BF16)[:, :head]

    outs = (ok1, ov1, ok2, ov2)

    def write_out(c):
        for t in range(groups):
            outs[c][t * WIDE:(t + 1) * WIDE, :] = recvb[c, :, t * WIDE:(t + 1) * WIDE].T

    unit = shot.shape[4]

    def block(which, at, n):
        return pl.ds(pl.multiple_of(which * half + at * unit, unit), n * unit)

    def put(ref, at, n, value):
        for k in range(n):
            ref[at + k] = value[:, k * unit:(k + 1) * unit].astype(BF16)

    def get(ref, at, n):
        return jnp.concatenate([ref[at + k].astype(F32) for k in range(n)], axis=1)

    def all_reduce(r, product, residual, between, parts, window):
        def send(ref, dst, ssem, rsem, peer):
            rcopy(ref, dst, ss_r.at[r, ssem], rs_r.at[r, rsem], peer).start()

        for q, (at, n) in enumerate(parts):
            put(part.at[r], at, n, product(1 - core, at, n))
            send(part.at[r, pl.ds(at, n)], d1.at[r, pl.ds(at, n)], 0, q, partner)
        for q, (at, n) in enumerate(parts):
            mine = product(core, at, n)
            with jax.named_scope("swap_wait"):
                drain(d1.at[r, pl.ds(at, n)], rs_r.at[r, q])
            put(shot.at[r, chip], at, n, mine + get(d1.at[r], at, n))
            piece = shot.at[r, chip, pl.ds(at, n)]
            for dx in (2, 1, 3):
                send(piece, piece, 1, 2 + q, device(dx, 0))
        with jax.named_scope("between"):
            between()
        for q, (at, n) in enumerate(parts):
            with jax.named_scope("shot_wait"):
                drain(shot.at[r, pl.ds(0, CHIPS - 1), pl.ds(at, n)], rs_r.at[r, 2 + q])
            total = (get(shot.at[r, 0], at, n) + get(shot.at[r, 1], at, n)) + (get(shot.at[r, 2], at, n) + get(shot.at[r, 3], at, n))
            put(fin.at[r, core], at, n, residual(at, n) + total)
            piece = fin.at[r, core, pl.ds(at, n)]
            send(piece, piece, 0, 4, partner)
        send_caches(window)
        with jax.named_scope("last_wait"):
            drain(fin.at[r, 1 - core], rs_r.at[r, 4])
        pieces = [fin[r, h, n].astype(F32) for h in range(2) for n in range(shot.shape[2])]
        return jnp.concatenate(pieces, axis=1)

    def gates(layer, m):
        logits = nt(wr[layer], m)
        e_i = iota((experts, rows), 0)
        chosen = e_i == choice[layer, 0:1, :]
        for n in range(1, choice.shape[1]):
            chosen = chosen | (e_i == choice[layer, n:n + 1, :])
        top = jnp.max(jnp.where(chosen, logits, -3e38), axis=0, keepdims=True)
        weight = jnp.where(chosen, jnp.exp(jnp.where(chosen, logits - top, 0.0)), 0.0)
        return (weight / jnp.sum(weight, axis=0, keepdims=True)).T

    def wait_weights(layer):
        for which, ref in enumerate((wg, wu, wd)):
            drain(ref.at[layer], sem_w.at[layer, which])

    def experts_up(layer, m):
        gate = gates(layer, m)
        pairs = step // LANES
        for c in range(CHUNKS):
            at = slice(c * step, (c + 1) * step)
            g = nt(m, wg[layer, at, :])
            up = nt(wu[layer, at, :], m).T
            wide = jnp.concatenate([jnp.where(left, gate[:, 2 * n:2 * n + 1], gate[:, 2 * n + 1:2 * n + 2]) for n in range(c * pairs, (c + 1) * pairs)], axis=1)
            ubuf[:, at] = (jax.nn.silu(g) * up * wide).astype(BF16)

    def send_caches(wanted):
        for c, n in wanted:
            a2a_copy(c, n).start()

    with jax.named_scope("small_wait"):
        for copy in small[1:4]:
            copy.wait()
    x = hid[...].astype(F32)
    with jax.named_scope("project"):
        q3 = project(0, x)
        queries = pack_queries(q3)
        qrecv[me] = queries.astype(BF16)
    with jax.named_scope("barrier"):
        pl.semaphore_wait(barrier, len(OFFSETS))
    for n in range(7):
        q_copy(n).start()
    with jax.named_scope("permute1"):
        loads[1].wait()
        permute(1)
    with jax.named_scope("permute_rest"):
        loads[0].wait()
        permute(0)
    send_caches(WINDOWS[0])
    with jax.named_scope("own_score"):
        own_score = half_sum(queries * pack_fresh(kdup[0])) * (head ** -0.5)
    with jax.named_scope("permute23"):
        for copy in small[4:]:
            copy.wait()
        for c in (2, 3):
            loads[c].wait()
            permute(c)
        for c in range(4):
            keep_own(c)
    with jax.named_scope("q_wait"):
        drain(seven(qrecv), rs_q)
    send_caches(WINDOWS[1])
    with jax.named_scope("local_scores"):
        local_scores()
    for n in range(7):
        p_copy(n).start()
    send_caches(WINDOWS[2])
    precv[me] = psend[me]
    with jax.named_scope("p_wait"):
        drain(seven(precv), rs_p)
    send_caches(WINDOWS[3])
    with jax.named_scope("merge"):
        s = gathered_scores(own_score)

    for layer in range(2):
        if layer:
            with jax.named_scope("project"):
                block_queries(project(layer, x))
            s = layer_scores(layer)
        first, second = attend(layer, s)
        n1 = first.shape[1]

        def out_product(which, at, n, layer=layer, first=first, second=second, n1=n1):
            cols = block(which, at, n)
            return nn(first, wo[layer, :n1, cols]) + nn(second, wo[layer, n1:, cols])

        def between_attn(layer=layer):
            if layer:
                write_out(2)
                write_out(3)
            else:
                write_out(1)
            wait_weights(layer)

        def between_moe(layer=layer):
            if layer:
                a2a_wait(0)
                for t in range(groups):
                    place_new(0, t, kdup, 0)
                write_out(0)

        def residual_attn(at, n, layer=layer):
            return get(fin.at[2 * layer - 1, core], at, n) if layer else hid[:, block(core, at, n)].astype(F32)

        x = all_reduce(2 * layer, out_product, residual_attn, between_attn, ((0, 3),), WINDOWS[4 + 2 * layer])
        m = norm(x, gm[layer:layer + 1, :])
        with jax.named_scope("up"):
            experts_up(layer, m)

        def down_product(which, at, n, layer=layer):
            with jax.named_scope("down"):
                return nn(ubuf[...], wd[layer, :, block(which, at, n)])

        def residual_moe(at, n, layer=layer):
            return get(fin.at[2 * layer, core], at, n)

        x = all_reduce(2 * layer + 1, down_product, residual_moe, between_moe, ((0, 2), (2, 1)), () if layer else WINDOWS[5])
    out_hid[...] = x.astype(BF16)

    with jax.named_scope("tail"):
        for r in range(4):
            drain(shot.at[r, pl.ds(0, 2)], ss_r.at[r, 0])
            drain(shot.at[r, pl.ds(0, CHIPS - 1)], ss_r.at[r, 1])
        drain(seven(qrecv), ss_q)
        drain(seven(psend), ss_p)
        for c in range(4):
            drain(sendb.at[c, pl.ds(0, len(OFFSETS))], ss_a.at[c])


def finish(*refs):
    n = len(refs) // 2
    copies = [pltpu.make_async_copy(refs[i], refs[n + i], refs[-1].at[i]) for i in range(n)]
    for copy in copies:
        copy.start()
    for copy in copies:
        copy.wait()


def solution(mesh):
    seq_spec = P('dp', 'tp', None, None)
    head_spec = P('dp', None, 'tp', None)
    col_spec = P(None, None, 'tp')
    ff_spec = P(None, None, None, 'tp')
    peers = mesh.shape['tp']

    def local_step(hidden, lengths, choice, keys_one, vals_one, keys_two, vals_two, g_attn, w_q, w_k, w_v, w_o, g_mlp, w_router, w_gate, w_up, w_down):
        rows, pos, heads, head = keys_one.shape
        dim = hidden.shape[1]
        layers, experts, ff = w_down.shape[:3]
        seq = pos * peers
        flat = lambda t: t.reshape(rows * pos * heads, head)
        turn = lambda t: jnp.swapaxes(t, -1, -2)
        wide = experts * ff
        any_spec = pl.BlockSpec(memory_space=pl.ANY)
        cache_shape = pltpu.VMEM((rows * head, seq), BF16)
        wqkv_rows = w_q.shape[2] + w_k.shape[2] + 2 * w_v.shape[2]
        scratch = [
            pltpu.SMEM((rows,), jnp.int32), pltpu.VMEM((rows, dim), BF16), pltpu.VMEM((layers, choice.shape[2], rows), jnp.int32),
            pltpu.VMEM((layers, dim), BF16), pltpu.VMEM((layers, dim), BF16),
            pltpu.VMEM((4, rows * pos * heads, head), BF16), pltpu.VMEM((4, heads, pos, rows * head), BF16),
            pltpu.VMEM((4, seq, rows * head), BF16),
            pltpu.VMEM((layers, wqkv_rows, dim), BF16), pltpu.VMEM((layers, w_o.shape[1], dim), BF16),
            pltpu.VMEM((layers, experts, dim), BF16),
            pltpu.VMEM((layers, wide, dim), BF16), pltpu.VMEM((layers, wide, dim), BF16), pltpu.VMEM((layers, wide, dim), BF16),
            pltpu.VMEM((LANES, WIDE), BF16), pltpu.VMEM((layers, rows, LANES), F32), pltpu.VMEM((layers, rows, LANES), F32), pltpu.VMEM((2, rows, LANES), F32),
            pltpu.VMEM((LANES, seq), F32), pltpu.VMEM((LANES, WIDE), F32),
            pltpu.VMEM((rows, wide), BF16),
            pltpu.VMEM((4, 3, rows, dim // 6), BF16), pltpu.VMEM((4, 3, rows, dim // 6), BF16),
            pltpu.VMEM((4, CHIPS, 3, rows, dim // 6), BF16), pltpu.VMEM((4, 2, 3, rows, dim // 6), BF16),
            pltpu.VMEM((heads, rows * 2, LANES), BF16), pltpu.VMEM((heads, TILE, LANES), F32), pltpu.VMEM((heads, TILE, LANES), F32),
            pltpu.SemaphoreType.DMA((7,)), pltpu.SemaphoreType.DMA((4,)), pltpu.SemaphoreType.DMA((layers, 3)),
            pltpu.SemaphoreType.DMA((layers,)),
            pltpu.SemaphoreType.DMA((4,)), pltpu.SemaphoreType.DMA((4,)),
            pltpu.SemaphoreType.DMA((4, 2)), pltpu.SemaphoreType.DMA((4, 5)),
            pltpu.SemaphoreType.DMA(()), pltpu.SemaphoreType.DMA(()), pltpu.SemaphoreType.DMA(()), pltpu.SemaphoreType.DMA(()),
        ]
        out = pl.pallas_call(
            kernel,
            name="decode_step",
            out_shape=(pltpu.VMEM((rows, dim), BF16),) + (cache_shape,) * 4,
            in_specs=[any_spec] * 17,
            out_specs=(pl.BlockSpec(memory_space=pltpu.VMEM),) * 5,
            scratch_shapes=scratch,
            compiler_params=pltpu.CompilerParams(collective_id=0, has_side_effects=True, vmem_limit_bytes=64800000),
        )(lengths, hidden, turn(choice), flat(keys_one), flat(vals_one), flat(keys_two), flat(vals_two), g_attn, turn(w_q), turn(w_k), turn(w_v), w_o,
          g_mlp, turn(w_router), turn(w_gate).reshape(layers, wide, dim), turn(w_up).reshape(layers, wide, dim), w_down.reshape(layers, wide, dim))
        out = pl.pallas_call(
            finish,
            name="finish",
            out_shape=[jax.ShapeDtypeStruct(t.shape, t.dtype) for t in out],
            in_specs=[pl.BlockSpec(memory_space=pltpu.VMEM)] * len(out),
            out_specs=[any_spec] * len(out),
            scratch_shapes=[pltpu.SemaphoreType.DMA((len(out),))],
            compiler_params=pltpu.CompilerParams(vmem_limit_bytes=1 << 20),
        )(*[pltpu.with_memory_space_constraint(t, pltpu.VMEM) for t in out])
        caches = [jnp.transpose(t.reshape(rows, head, seq), (0, 2, 1))[:, :, None, :] for t in out[1:]]
        return (out[0], *caches)

    return jax.shard_map(local_step, mesh=mesh, in_specs=(P('dp', None), P('dp'), P(None, 'dp', None), seq_spec, seq_spec, seq_spec, seq_spec, P(), col_spec, col_spec, col_spec, P(None, 'tp', None), P(), P(), ff_spec, ff_spec, P(None, None, 'tp', None)), out_specs=(P('dp', None), head_spec, head_spec, head_spec, head_spec), check_vma=False)
```

```python
import functools

import jax
import jax.numpy as jnp
from jax import lax
from jax.experimental import pallas as pl
from jax.experimental.pallas import tpu as pltpu
from jax.sharding import PartitionSpec as P

EPS = 1e-5
THETA = 1000000.0
MESH = pl.DeviceIdType.MESH
F32 = jnp.float32
BF16 = jnp.bfloat16
LANES, WIDE, TILE, HEAD = 128, 256, 16, 64
CHIPS = 4
OFFSETS = ((2, 0), (2, 1), (1, 0), (3, 0), (1, 1), (3, 1), (0, 1))
def units(cache, *which):
    pairs = ((0,), (1,), (2, 3), (4, 5), (6,))
    return [(cache, n) for k in which for n in pairs[k]]


WINDOWS = (
    units(1, 2, 3, 0, 1, 4),
    [],
    units(3, 4) + units(2, 4, 0, 1),
    units(2, 2),
    units(2, 3) + units(3, 0, 1, 2, 3),
    units(0, 4, 0, 1),
    units(0, 2, 3),
)
CHUNKS = 10


def nt(lhs, rhs):
    return lax.dot_general(lhs, rhs, (((1,), (1,)), ((), ())), preferred_element_type=F32)


def nn(lhs, rhs):
    return jnp.dot(lhs, rhs, preferred_element_type=F32)


def iota(shape, dim):
    return lax.broadcasted_iota(jnp.int32, shape, dim)


def kernel(len_h, hid_h, choice_h, k1_h, v1_h, k2_h, v2_h, ga_h, wq_h, wk_h, wv_h, wo_h, gm_h, wr_h, wg_h, wu_h, wd_h,
           out_hid, ok1, ov1, ok2, ov2,
           len_s, hid, choice, ga, gm, xst, sendb, recvb, wqkv, wo, wr, wg, wu, wd,
           qall, kdup, vdup, turns, sc, ov, ubuf, part, d1, shot, fin, qrecv, psend, precv,
           sem_small, sem_x, sem_w, sem_wqkv, ss_a, rs_a, ss_r, rs_r, ss_q, rs_q, ss_p, rs_p):
    rows, dim = hid.shape
    half = dim // 2
    seq = recvb.shape[1]
    pos = seq // (2 * CHIPS)
    lanes = recvb.shape[2]
    groups = lanes // WIDE
    head = HEAD
    experts = wr.shape[1]
    step = wg.shape[1] // CHUNKS

    me = lax.axis_index("tp")
    chip, core = me // 2, lax.rem(me, 2)
    partner = chip * 2 + 1 - core

    def device(dx, flip):
        return lax.rem(chip + dx, CHIPS) * 2 + (1 - core if flip else core)

    def rcopy(src, dst, ssem, rsem, peer):
        return pltpu.make_async_remote_copy(src, dst, ssem, rsem, device_id={"tp": peer}, device_id_type=MESH)

    def drain(ref, sem):
        pltpu.make_async_copy(ref, ref, sem).wait()

    loads = [pltpu.make_async_copy(src, xst.at[c], sem_x.at[c]) for c, src in enumerate((k1_h, v1_h, k2_h, v2_h))]
    small = [pltpu.make_async_copy(src, dst, sem_small.at[n]) for n, (src, dst) in enumerate(
        ((len_h, len_s), (hid_h, hid), (ga_h, ga), (gm_h, gm), (choice_h, choice), (wr_h, wr), (wo_h, wo)))]

    def qkv_loads(layer):
        nq, nk = wq_h.shape[1], wk_h.shape[1]
        return [pltpu.make_async_copy(src.at[layer], wqkv.at[layer, pl.ds(at, size)], sem_wqkv.at[layer])
                for src, at, size in ((wq_h, 0, nq), (wk_h, nq, nk), (wv_h, nq + nk, nk), (wv_h, nq + 2 * nk, nk))]

    for copy in small[:2]:
        copy.start()
    for copy in qkv_loads(0):
        copy.start()
    for copy in small[2:4]:
        copy.start()
    barrier = pltpu.get_barrier_semaphore()
    for dx, flip in OFFSETS:
        pl.semaphore_signal(barrier, inc=1, device_id={"tp": device(dx, flip)}, device_id_type=MESH)
    for c in (1, 0, 2, 3):
        loads[c].start()
    for copy in small[4:]:
        copy.start()
    for copy in qkv_loads(1):
        copy.start()

    def w_copy(layer, which, c):
        src, dst = ((wg_h, wg), (wu_h, wu), (wd_h, wd))[which]
        at = pl.ds(pl.multiple_of(c * step, step), step)
        return pltpu.make_async_copy(src.at[layer, at], dst.at[layer, at], sem_w.at[layer, which])

    def permute(c):
        i, j = iota((LANES, LANES), 0), iota((LANES, LANES), 1)
        perm = (j == lax.rem(i, TILE) * 8 + i // TILE).astype(BF16)

        for t in range(groups):
            tiles = [xst[c, slice(t * 512 + n * LANES, t * 512 + n * LANES + LANES), :] for n in range(4)]
            moved = nn(perm, jnp.concatenate(tiles, axis=1)).astype(BF16)
            sendb[c, :, :, slice(t * WIDE, t * WIDE + WIDE)] = moved.reshape(8, pos, WIDE)

    def a2a_copy(c, n):
        peer = device(*OFFSETS[n])
        return rcopy(sendb.at[c, peer], recvb.at[c, pl.ds(pl.multiple_of(me * pos, pos), pos)], ss_a.at[c], rs_a.at[c], peer)

    def a2a_wait(c):
        drain(recvb.at[c, pl.ds(0, len(OFFSETS) * pos)], rs_a.at[c])

    def keep_own(c):
        recvb[c, pl.ds(pl.multiple_of(me * pos, pos), pos), :] = sendb[c, me]

    for layer in range(2):
        def start_weights(c, _, layer=layer):
            w_copy(layer, 0, c).start()
            w_copy(layer, 1, c).start()
            w_copy(layer, 2, c).start()
            return 0
        lax.fori_loop(0, CHUNKS, start_weights, 0)

    with jax.named_scope("len_wait"):
        small[0].wait()
    lane = iota((rows, LANES), 1)
    row = iota((rows, LANES), 0)
    len_f = jnp.zeros((rows, LANES), F32)
    for b in range(rows):
        len_f = jnp.where(row == b, len_s[b].astype(F32), len_f)
    freq = jnp.exp(lax.rem(lane, 32).astype(F32) * (-2.0 / head * 13.815510557964274))
    angle = len_f * freq
    turns[0], turns[1] = jnp.cos(angle), jnp.sin(angle)
    low = lax.rem(lane, head) < head // 2
    left = lane < head

    def rope(x):
        turned = jnp.where(low, -pltpu.roll(x, 96, 1), pltpu.roll(x, 32, 1))
        return (x * turns[0] + turned * turns[1]).astype(BF16).astype(F32)

    def norm(x, gain):
        scale = lax.rsqrt(jnp.mean(x * x, axis=-1, keepdims=True) + EPS)
        return (x * scale * gain.astype(F32)).astype(BF16)

    def project(layer, x):
        drain(wqkv.at[layer], sem_wqkv.at[layer])
        qkv = nt(norm(x, ga[layer:layer + 1, :]), wqkv[layer])
        t0, t1 = rope(qkv[:, :LANES]), rope(qkv[:, LANES:WIDE])
        s0, s1 = pltpu.roll(t0, HEAD, 1), pltpu.roll(t1, HEAD, 1)
        q3 = jnp.concatenate([jnp.where(left, t0, s0), jnp.where(left, s0, t0), jnp.where(left, t1, s1)], axis=0).astype(BF16)
        kdup[layer] = jnp.where(left, s1, t1)
        vdup[layer] = qkv[:, WIDE:384].astype(BF16).astype(F32)
        return q3

    def block_queries(q3):
        i, j = iota((LANES, 96), 0), iota((LANES, 96), 1)
        slot = lax.rem(i, TILE)
        pick = (lax.rem(slot, 4) < 3) & (j == lax.rem(slot, 4) * rows + i // 4)
        dup = nn(pick.astype(BF16), q3)
        slot2, lane2 = lax.rem(iota((LANES, WIDE), 0), TILE), iota((LANES, WIDE), 1)
        both = jnp.concatenate([dup, dup], axis=1)
        qall[...] = jnp.where(slot2 // 4 == lane2 // HEAD, both, 0.0).astype(BF16)

    hb = rows // 2
    prow, plane = iota((hb * 4, LANES), 0), iota((hb * 4, LANES), 1)
    pleft = plane < head

    def pack(table, cells):
        width = table.shape[0]
        i, j = iota((hb * 4, width), 0), iota((hb * 4, width), 1)
        low_half = nn(cells(i, j, 0).astype(BF16), table)
        high_half = nn(cells(i, j, hb).astype(BF16), table)
        return jnp.where(pleft, low_half, high_half)

    def pack_queries(q3):
        return pack(q3, lambda i, j, b0: (lax.rem(i, 4) < 3) & (j == lax.rem(i, 4) * rows + i // 4 + b0))

    def pack_fresh(table):
        return pack(table.astype(BF16), lambda i, j, b0: j == i // 4 + b0)

    def to_all(n, src, dst, ssem, rsem):
        return rcopy(src, dst, ssem, rsem, device(*OFFSETS[n]))

    def q_copy(n):
        return to_all(n, qrecv.at[me], qrecv.at[me], ss_q, rs_q)

    def p_copy(n):
        return to_all(n, psend.at[device(*OFFSETS[n])], precv.at[me], ss_p, rs_p)

    def seven(ref):
        return ref.at[pl.ds(0, len(OFFSETS))]

    def local_scores():
        wide_row, wide_lane = iota((LANES, WIDE), 0), iota((LANES, WIDE), 1)
        diagonal = wide_lane // head == lax.rem(wide_row, TILE) // 4
        half_lane = iota((LANES, LANES), 1) < head
        lane_block = iota((TILE, LANES), 1) // pos
        kept = [jnp.zeros((TILE, LANES), F32)] * 8
        for t in range(groups):
            at = slice(t % 4 * TILE, t % 4 * TILE + TILE)
            q = qrecv[:, at, :].reshape(LANES, LANES).astype(F32)
            q = jnp.where(half_lane if t < 4 else ~half_lane, q, 0.0)
            q = q + pltpu.roll(q, HEAD, 1)
            q = jnp.where(diagonal, jnp.concatenate([q, q], axis=1), 0.0).astype(BF16)
            keys = sendb[0, :, :, t * WIDE:(t + 1) * WIDE].reshape(LANES, WIDE)
            s = nt(q, keys) * (head ** -0.5)
            for h in range(8):
                turned = s[h * TILE:(h + 1) * TILE, :]
                if h != t:
                    turned = pltpu.roll(turned, (t - h) % 8 * pos, 1)
                kept[h] = jnp.where(lane_block == t, turned, kept[h])
        for h in range(8):
            psend[h] = kept[h]

    def half_sum(x):
        low_half = jnp.sum(jnp.where(pleft, x, 0.0), axis=-1, keepdims=True)
        high_half = jnp.sum(jnp.where(pleft, 0.0, x), axis=-1, keepdims=True)
        return jnp.where(pleft, low_half, high_half)

    def gathered_scores(own):
        lane_block = iota((TILE, LANES), 1) // pos
        for t in range(groups):
            tile = precv[t]
            for j in range(2 * CHIPS):
                turned = precv[j]
                if j != t:
                    turned = pltpu.roll(turned, (j - t) % 8 * pos, 1)
                tile = jnp.where(lane_block == j, turned, tile)
            sc[t * TILE:(t + 1) * TILE, :] = tile
        fresh = jnp.concatenate([own[:, :1], own[:, head:head + 1]], axis=0)
        limit = jnp.zeros((LANES, LANES), jnp.int32)
        row_i, lane_i = iota((LANES, LANES), 0) // 4, iota((LANES, LANES), 1)
        for b in range(rows):
            limit = jnp.where(row_i == b, len_s[b], limit)
        s = jnp.where(lane_i == limit, fresh, sc[...])
        return jnp.where(lane_i <= limit, s, -1e30)

    def place_new(c, t, fresh, layer):
        at = slice(t * WIDE, t * WIDE + WIDE)
        pos_i, lane_i = iota((seq, LANES), 0), iota((seq, LANES), 1)
        pieces = []
        for n in range(2):
            first = t * 4 + 2 * n
            where_new = jnp.where(lane_i < head, len_s[first], len_s[first + 1])
            line = jnp.where(lane_i[:1] < head, fresh[layer, first:first + 1, :], fresh[layer, first + 1:first + 2, :])
            old = recvb[c, :, slice(t * WIDE + n * LANES, t * WIDE + n * LANES + LANES)].astype(F32)
            pieces.append(jnp.where(pos_i == where_new, line, old))
        tile = jnp.concatenate(pieces, axis=1).astype(BF16)
        recvb[c, :, at] = tile
        return tile

    def layer_scores(layer):
        ck = 2 * layer
        with jax.named_scope("wait_keys"):
            a2a_wait(ck)

        def scores(t):
            tile = place_new(ck, t, kdup, layer)
            at = slice(t * TILE, t * TILE + TILE)
            s = nt(qall[at, :], tile) * (head ** -0.5)
            slot, p = iota((TILE, seq), 0) // 4, iota((TILE, seq), 1)
            limit = jnp.where(slot == 0, len_s[4 * t], jnp.where(slot == 1, len_s[4 * t + 1], jnp.where(slot == 2, len_s[4 * t + 2], len_s[4 * t + 3])))
            sc[at, :] = jnp.where(p <= limit, s, -1e30)
        with jax.named_scope("scores"):
            for t in range(groups):
                scores(t)
        return sc[...]

    def attend(layer, s):
        cv = 2 * layer + 1
        e = jnp.exp(s - jnp.max(s, axis=-1, keepdims=True))
        sc[...] = e / jnp.sum(e, axis=-1, keepdims=True)
        with jax.named_scope("wait_values"):
            a2a_wait(cv)

        def values(t):
            tile = place_new(cv, t, vdup, layer)
            at = slice(t * TILE, t * TILE + TILE)
            ov[at, :] = nn(sc[at, :].astype(BF16), tile)
        with jax.named_scope("values"):
            for t in range(groups):
                values(t)
        slot2, lane2 = lax.rem(iota((LANES, WIDE), 0), TILE), iota((LANES, WIDE), 1)
        kept = jnp.where(slot2 // 4 == lane2 // HEAD, ov[...], 0.0)
        both = (kept[:, :LANES] + kept[:, LANES:]).astype(BF16)
        i, j = iota((rows, LANES), 0), iota((rows, LANES), 1)
        per_head = []
        for r in range(3):
            got = nn((j == i * 4 + r).astype(BF16), both)
            per_head.append(got + pltpu.roll(got, HEAD, 1))
        return jnp.where(left, per_head[0], per_head[1]).astype(BF16), per_head[2].astype(BF16)[:, :head]

    outs = (ok1, ov1, ok2, ov2)

    def write_out(c):
        for t in range(groups):
            outs[c][t * WIDE:(t + 1) * WIDE, :] = recvb[c, :, t * WIDE:(t + 1) * WIDE].T

    unit = shot.shape[4]

    def block(which, at, n):
        return pl.ds(pl.multiple_of(which * half + at * unit, unit), n * unit)

    def put(ref, at, n, value):
        for k in range(n):
            ref[at + k] = value[:, k * unit:(k + 1) * unit].astype(BF16)

    def get(ref, at, n):
        return jnp.concatenate([ref[at + k].astype(F32) for k in range(n)], axis=1)

    def all_reduce(r, product, residual, between, parts, window):
        def send(ref, dst, ssem, rsem, peer):
            rcopy(ref, dst, ss_r.at[ssem], rs_r.at[r, rsem], peer).start()

        for q, (at, n) in enumerate(parts):
            put(part.at[r], at, n, product(1 - core, at, n))
            send(part.at[r, pl.ds(at, n)], d1.at[r, pl.ds(at, n)], 0, q, partner)
        for q, (at, n) in enumerate(parts):
            mine = product(core, at, n)
            with jax.named_scope("swap_wait"):
                drain(d1.at[r, pl.ds(at, n)], rs_r.at[r, q])
            put(shot.at[r, chip], at, n, mine + get(d1.at[r], at, n))
            piece = shot.at[r, chip, pl.ds(at, n)]
            for dx in (2, 1, 3):
                send(piece, piece, 1, 2 + q, device(dx, 0))
        with jax.named_scope("between"):
            between()
        for q, (at, n) in enumerate(parts):
            with jax.named_scope("shot_wait"):
                drain(shot.at[r, pl.ds(0, CHIPS - 1), pl.ds(at, n)], rs_r.at[r, 2 + q])
            total = (get(shot.at[r, 0], at, n) + get(shot.at[r, 1], at, n)) + (get(shot.at[r, 2], at, n) + get(shot.at[r, 3], at, n))
            put(fin.at[r, core], at, n, residual(at, n) + total)
            piece = fin.at[r, core, pl.ds(at, n)]
            send(piece, piece, 0, 4, partner)
        send_caches(window)
        with jax.named_scope("last_wait"):
            drain(fin.at[r, 1 - core], rs_r.at[r, 4])
        pieces = [fin[r, h, n].astype(F32) for h in range(2) for n in range(shot.shape[2])]
        return jnp.concatenate(pieces, axis=1)

    def gates(layer, m):
        logits = nt(wr[layer], m)
        e_i = iota((experts, rows), 0)
        chosen = e_i == choice[layer, 0:1, :]
        for n in range(1, choice.shape[1]):
            chosen = chosen | (e_i == choice[layer, n:n + 1, :])
        top = jnp.max(jnp.where(chosen, logits, -3e38), axis=0, keepdims=True)
        weight = jnp.where(chosen, jnp.exp(jnp.where(chosen, logits - top, 0.0)), 0.0)
        return (weight / jnp.sum(weight, axis=0, keepdims=True)).T

    def wait_weights(layer):
        for which, ref in enumerate((wg, wu, wd)):
            drain(ref.at[layer], sem_w.at[layer, which])

    def experts_up(layer, m):
        gate = gates(layer, m)
        pairs = step // LANES
        for c in range(CHUNKS):
            at = slice(c * step, (c + 1) * step)
            g = nt(m, wg[layer, at, :])
            up = nt(wu[layer, at, :], m).T
            wide = jnp.concatenate([jnp.where(left, gate[:, 2 * n:2 * n + 1], gate[:, 2 * n + 1:2 * n + 2]) for n in range(c * pairs, (c + 1) * pairs)], axis=1)
            ubuf[:, at] = (jax.nn.silu(g) * up * wide).astype(BF16)

    def send_caches(wanted):
        for c, n in wanted:
            a2a_copy(c, n).start()

    with jax.named_scope("small_wait"):
        for copy in small[1:4]:
            copy.wait()
    x = hid[...].astype(F32)
    with jax.named_scope("project"):
        q3 = project(0, x)
        queries = pack_queries(q3)
        qrecv[me] = queries.astype(BF16)
    with jax.named_scope("barrier"):
        pl.semaphore_wait(barrier, len(OFFSETS))
    for n in range(7):
        q_copy(n).start()
    with jax.named_scope("permute1"):
        loads[1].wait()
        permute(1)
    with jax.named_scope("permute_rest"):
        loads[0].wait()
        permute(0)
    send_caches(WINDOWS[0])
    with jax.named_scope("own_score"):
        own_score = half_sum(queries * pack_fresh(kdup[0])) * (head ** -0.5)
    with jax.named_scope("permute23"):
        for copy in small[4:]:
            copy.wait()
        for c in (2, 3):
            loads[c].wait()
            permute(c)
        for c in range(4):
            keep_own(c)
    with jax.named_scope("q_wait"):
        drain(seven(qrecv), rs_q)
    send_caches(WINDOWS[1])
    with jax.named_scope("local_scores"):
        local_scores()
    for n in range(7):
        p_copy(n).start()
    send_caches(WINDOWS[2])
    precv[me] = psend[me]
    with jax.named_scope("p_wait"):
        drain(seven(precv), rs_p)
    send_caches(WINDOWS[3])
    with jax.named_scope("merge"):
        s = gathered_scores(own_score)

    for layer in range(2):
        if layer:
            with jax.named_scope("project"):
                block_queries(project(layer, x))
            s = layer_scores(layer)
        first, second = attend(layer, s)
        n1 = first.shape[1]

        def out_product(which, at, n, layer=layer, first=first, second=second, n1=n1):
            cols = block(which, at, n)
            return nn(first, wo[layer, :n1, cols]) + nn(second, wo[layer, n1:, cols])

        def between_attn(layer=layer):
            if layer:
                write_out(2)
                write_out(3)
            else:
                write_out(1)
            wait_weights(layer)

        def between_moe(layer=layer):
            if layer:
                a2a_wait(0)
                for t in range(groups):
                    place_new(0, t, kdup, 0)
                write_out(0)

        def residual_attn(at, n, layer=layer):
            return get(fin.at[2 * layer - 1, core], at, n) if layer else hid[:, block(core, at, n)].astype(F32)

        x = all_reduce(2 * layer, out_product, residual_attn, between_attn, ((0, 3),), WINDOWS[4 + 2 * layer])
        m = norm(x, gm[layer:layer + 1, :])
        with jax.named_scope("up"):
            experts_up(layer, m)

        def down_product(which, at, n, layer=layer):
            with jax.named_scope("down"):
                return nn(ubuf[...], wd[layer, :, block(which, at, n)])

        def residual_moe(at, n, layer=layer):
            return get(fin.at[2 * layer, core], at, n)

        x = all_reduce(2 * layer + 1, down_product, residual_moe, between_moe, ((0, 2), (2, 1)), () if layer else WINDOWS[5])
    out_hid[...] = x.astype(BF16)

    with jax.named_scope("tail"):
        drain(shot.at[:, pl.ds(0, 2)], ss_r.at[0])
        drain(shot.at[:, pl.ds(0, CHIPS - 1)], ss_r.at[1])
        drain(seven(qrecv), ss_q)
        drain(seven(psend), ss_p)
        for c in range(4):
            drain(sendb.at[c, pl.ds(0, len(OFFSETS))], ss_a.at[c])


def finish(*refs):
    n = len(refs) // 2
    copies = [pltpu.make_async_copy(refs[i], refs[n + i], refs[-1].at[i]) for i in range(n)]
    for copy in copies:
        copy.start()
    for copy in copies:
        copy.wait()


def solution(mesh):
    seq_spec = P('dp', 'tp', None, None)
    head_spec = P('dp', None, 'tp', None)
    col_spec = P(None, None, 'tp')
    ff_spec = P(None, None, None, 'tp')
    peers = mesh.shape['tp']

    def local_step(hidden, lengths, choice, keys_one, vals_one, keys_two, vals_two, g_attn, w_q, w_k, w_v, w_o, g_mlp, w_router, w_gate, w_up, w_down):
        rows, pos, heads, head = keys_one.shape
        dim = hidden.shape[1]
        layers, experts, ff = w_down.shape[:3]
        seq = pos * peers
        flat = lambda t: t.reshape(rows * pos * heads, head)
        turn = lambda t: jnp.swapaxes(t, -1, -2)
        wide = experts * ff
        any_spec = pl.BlockSpec(memory_space=pl.ANY)
        cache_shape = pltpu.VMEM((rows * head, seq), BF16)
        wqkv_rows = w_q.shape[2] + w_k.shape[2] + 2 * w_v.shape[2]
        scratch = [
            pltpu.SMEM((rows,), jnp.int32), pltpu.VMEM((rows, dim), BF16), pltpu.VMEM((layers, choice.shape[2], rows), jnp.int32),
            pltpu.VMEM((layers, dim), BF16), pltpu.VMEM((layers, dim), BF16),
            pltpu.VMEM((4, rows * pos * heads, head), BF16), pltpu.VMEM((4, heads, pos, rows * head), BF16),
            pltpu.VMEM((4, seq, rows * head), BF16),
            pltpu.VMEM((layers, wqkv_rows, dim), BF16), pltpu.VMEM((layers, w_o.shape[1], dim), BF16),
            pltpu.VMEM((layers, experts, dim), BF16),
            pltpu.VMEM((layers, wide, dim), BF16), pltpu.VMEM((layers, wide, dim), BF16), pltpu.VMEM((layers, wide, dim), BF16),
            pltpu.VMEM((LANES, WIDE), BF16), pltpu.VMEM((layers, rows, LANES), F32), pltpu.VMEM((layers, rows, LANES), F32), pltpu.VMEM((2, rows, LANES), F32),
            pltpu.VMEM((LANES, seq), F32), pltpu.VMEM((LANES, WIDE), F32),
            pltpu.VMEM((rows, wide), BF16),
            pltpu.VMEM((4, 3, rows, dim // 6), BF16), pltpu.VMEM((4, 3, rows, dim // 6), BF16),
            pltpu.VMEM((4, CHIPS, 3, rows, dim // 6), BF16), pltpu.VMEM((4, 2, 3, rows, dim // 6), BF16),
            pltpu.VMEM((heads, rows * 2, LANES), BF16), pltpu.VMEM((heads, TILE, LANES), F32), pltpu.VMEM((heads, TILE, LANES), F32),
            pltpu.SemaphoreType.DMA((7,)), pltpu.SemaphoreType.DMA((4,)), pltpu.SemaphoreType.DMA((layers, 3)),
            pltpu.SemaphoreType.DMA((layers,)),
            pltpu.SemaphoreType.DMA((4,)), pltpu.SemaphoreType.DMA((4,)),
            pltpu.SemaphoreType.DMA((2,)), pltpu.SemaphoreType.DMA((4, 5)),
            pltpu.SemaphoreType.DMA(()), pltpu.SemaphoreType.DMA(()), pltpu.SemaphoreType.DMA(()), pltpu.SemaphoreType.DMA(()),
        ]
        out = pl.pallas_call(
            kernel,
            name="decode_step",
            out_shape=(pltpu.VMEM((rows, dim), BF16),) + (cache_shape,) * 4,
            in_specs=[any_spec] * 17,
            out_specs=(pl.BlockSpec(memory_space=pltpu.VMEM),) * 5,
            scratch_shapes=scratch,
            compiler_params=pltpu.CompilerParams(collective_id=0, has_side_effects=True, vmem_limit_bytes=64800000),
        )(lengths, hidden, turn(choice), flat(keys_one), flat(vals_one), flat(keys_two), flat(vals_two), g_attn, turn(w_q), turn(w_k), turn(w_v), w_o,
          g_mlp, turn(w_router), turn(w_gate).reshape(layers, wide, dim), turn(w_up).reshape(layers, wide, dim), w_down.reshape(layers, wide, dim))
        out = pl.pallas_call(
            finish,
            name="finish",
            out_shape=[jax.ShapeDtypeStruct(t.shape, t.dtype) for t in out],
            in_specs=[pl.BlockSpec(memory_space=pltpu.VMEM)] * len(out),
            out_specs=[any_spec] * len(out),
            scratch_shapes=[pltpu.SemaphoreType.DMA((len(out),))],
            compiler_params=pltpu.CompilerParams(vmem_limit_bytes=1 << 20),
        )(*[pltpu.with_memory_space_constraint(t, pltpu.VMEM) for t in out])
        caches = [jnp.transpose(t.reshape(rows, head, seq), (0, 2, 1))[:, :, None, :] for t in out[1:]]
        return (out[0], *caches)

    return jax.shard_map(local_step, mesh=mesh, in_specs=(P('dp', None), P('dp'), P(None, 'dp', None), seq_spec, seq_spec, seq_spec, seq_spec, P(), col_spec, col_spec, col_spec, P(None, 'tp', None), P(), P(), ff_spec, ff_spec, P(None, None, 'tp', None)), out_specs=(P('dp', None), head_spec, head_spec, head_spec, head_spec), check_vma=False)
```
